64 devices in a mesh: dp: 4 (over x, y), tp: 16 (over z, core).
Axes of the slice: x: 2, y: 2, z: 8, core: 2. Of those that a mesh axis runs over, the one named last changes fastest.
The devices are a block of a 4x4x8 slice.
Arguments:
- x_tokens: bfloat16 [8192, 2048], P(('dp', 'tp')), parts along dimension 0
- dy_tokens: bfloat16 [8192, 2048], P(('dp', 'tp')), parts along dimension 0
- w_q: bfloat16 [2048, 16, 128], P(None, 'tp')
- w_k: bfloat16 [2048, 2, 128], replicated
- w_v: bfloat16 [2048, 2, 128], replicated
- w_o: bfloat16 [16, 128, 2048], P('tp')
- w_gate: bfloat16 [2048, 11008], P(None, 'tp')
- w_up: bfloat16 [2048, 11008], P(None, 'tp')
- w_down: bfloat16 [11008, 2048], P('tp')
Outputs:
- output 1: bfloat16 [8192, 2048], P(('dp', 'tp')), parts along dimension 0
- output 2: float32 [8192, 16, 128], P('dp', 'tp'), parts along dimension 0
- output 3: float32 [64, 256, 128], P(('dp', 'tp')), parts along dimension 0
- output 4: float32 [64, 256, 128], P(('dp', 'tp')), parts along dimension 0
- output 5: float32 [64, 128, 2048], P(('dp', 'tp')), parts along dimension 0
- output 6: float32 [8192, 11008], P('dp', 'tp'), parts along dimension 0
- output 7: float32 [8192, 11008], P('dp', 'tp'), parts along dimension 0
- output 8: float32 [44032, 2048], P(('dp', 'tp')), parts along dimension 0
There are 4 independent parts. The reference program is written for one: setup_inputs(seed, part) draws one part's arguments, and reference() takes and returns one part's arrays. A program takes and returns all parts, laid end to end along the dimension named above; an argument that names none is the same for every part.
All inputs are finite; a program needn't handle non-finite values.
Results may differ from the reference program's by a relative error of at most 0.0166535.
Values are sent between devices in bfloat16 or wider.
A program may use at most 768 MiB of HBM per device.

```python
import jax
import jax.numpy as jnp
from jax import lax

SEQ_LEN = 2048
D_MODEL = 2048
Q_HEADS = 16
KV_HEADS = 2
HEAD_DIM = 128
FF_DIM = 11008
TP_SIZE = 16


def setup_inputs(seed: int = 0, part: int = 0) -> dict:
    part_key = jax.random.fold_in(jax.random.key(seed), part)
    token_keys = jax.random.split(part_key, 2)
    weight_keys = jax.random.split(jax.random.key(seed + 1), 7)
    model_scale = D_MODEL ** -0.5
    x_tokens = jax.random.normal(token_keys[0], (SEQ_LEN, D_MODEL), jnp.float32).astype(jnp.bfloat16)
    dy_tokens = jax.random.normal(token_keys[1], (SEQ_LEN, D_MODEL), jnp.float32).astype(jnp.bfloat16)
    w_q = (jax.random.normal(weight_keys[0], (D_MODEL, Q_HEADS, HEAD_DIM), jnp.float32) * model_scale).astype(jnp.bfloat16)
    w_k = (jax.random.normal(weight_keys[1], (D_MODEL, KV_HEADS, HEAD_DIM), jnp.float32) * model_scale).astype(jnp.bfloat16)
    w_v = (jax.random.normal(weight_keys[2], (D_MODEL, KV_HEADS, HEAD_DIM), jnp.float32) * model_scale).astype(jnp.bfloat16)
    w_o = (jax.random.normal(weight_keys[3], (Q_HEADS, HEAD_DIM, D_MODEL), jnp.float32) * (Q_HEADS * HEAD_DIM) ** -0.5).astype(jnp.bfloat16)
    w_gate = (jax.random.normal(weight_keys[4], (D_MODEL, FF_DIM), jnp.float32) * model_scale).astype(jnp.bfloat16)
    w_up = (jax.random.normal(weight_keys[5], (D_MODEL, FF_DIM), jnp.float32) * model_scale).astype(jnp.bfloat16)
    w_down = (jax.random.normal(weight_keys[6], (FF_DIM, D_MODEL), jnp.float32) * FF_DIM ** -0.5).astype(jnp.bfloat16)
    return {"x_tokens": x_tokens, "dy_tokens": dy_tokens, "w_q": w_q, "w_k": w_k, "w_v": w_v, "w_o": w_o, "w_gate": w_gate, "w_up": w_up, "w_down": w_down}


def head_grads(operands):
    q_one, k_one, v_one, do_one = operands
    score_scale = HEAD_DIM ** -0.5
    positions = jnp.arange(SEQ_LEN)
    causal = positions[:, None] >= positions[None, :]
    scores = jnp.dot(q_one, k_one.T, preferred_element_type=jnp.float32) * score_scale
    scores = jnp.where(causal, scores, -jnp.inf)
    attn_prob = jax.nn.softmax(scores, axis=-1)
    prob_low = attn_prob.astype(jnp.bfloat16)
    out_one = jnp.dot(prob_low, v_one, preferred_element_type=jnp.float32).astype(jnp.bfloat16)
    d_prob = jnp.dot(do_one, v_one.T, preferred_element_type=jnp.float32)
    row_delta = jnp.sum(do_one.astype(jnp.float32) * out_one.astype(jnp.float32), axis=-1, keepdims=True)
    d_scores = (attn_prob * (d_prob - row_delta)).astype(jnp.bfloat16)
    dq_one = (jnp.dot(d_scores, k_one, preferred_element_type=jnp.float32) * score_scale).astype(jnp.bfloat16)
    dk_one = jnp.dot(d_scores.T, q_one, preferred_element_type=jnp.float32) * score_scale
    dv_one = jnp.dot(prob_low.T, do_one, preferred_element_type=jnp.float32)
    return out_one, dq_one, dk_one, dv_one


def reference(x_tokens, dy_tokens, w_q, w_k, w_v, w_o, w_gate, w_up, w_down):
    group_size = Q_HEADS // KV_HEADS
    replicas = TP_SIZE // KV_HEADS
    d_block = D_MODEL // replicas
    x_f32 = x_tokens.astype(jnp.float32)
    dy_f32 = dy_tokens.astype(jnp.float32)
    q_heads = jnp.einsum("td,dhe->hte", x_f32, w_q.astype(jnp.float32)).astype(jnp.bfloat16)
    k_heads = jnp.einsum("td,dge->gte", x_f32, w_k.astype(jnp.float32)).astype(jnp.bfloat16)
    v_heads = jnp.einsum("td,dge->gte", x_f32, w_v.astype(jnp.float32)).astype(jnp.bfloat16)
    do_heads = jnp.einsum("tc,hec->hte", dy_f32, w_o.astype(jnp.float32)).astype(jnp.bfloat16)
    k_rep = jnp.repeat(k_heads, group_size, axis=0)
    v_rep = jnp.repeat(v_heads, group_size, axis=0)
    out_heads, dq_heads, dk_heads, dv_heads = lax.map(head_grads, (q_heads, k_rep, v_rep, do_heads))
    dk_sum = dk_heads.reshape(KV_HEADS, group_size, SEQ_LEN, HEAD_DIM).sum(axis=1).astype(jnp.bfloat16).astype(jnp.float32)
    dv_sum = dv_heads.reshape(KV_HEADS, group_size, SEQ_LEN, HEAD_DIM).sum(axis=1).astype(jnp.bfloat16).astype(jnp.float32)
    dq_f32 = dq_heads.astype(jnp.float32)
    dw_o = jnp.einsum("hte,tc->hec", out_heads.astype(jnp.float32), dy_f32)
    dw_q = jnp.einsum("td,hte->dhe", x_f32, dq_f32)
    x_split = x_f32.reshape(SEQ_LEN, replicas, d_block)
    dw_k = jnp.einsum("trd,gte->grde", x_split, dk_sum).reshape(TP_SIZE, d_block, HEAD_DIM)
    dw_v = jnp.einsum("trd,gte->grde", x_split, dv_sum).reshape(TP_SIZE, d_block, HEAD_DIM)
    gate_pre = jnp.dot(x_tokens, w_gate, preferred_element_type=jnp.float32).astype(jnp.bfloat16).astype(jnp.float32)
    up_pre = jnp.dot(x_tokens, w_up, preferred_element_type=jnp.float32).astype(jnp.bfloat16).astype(jnp.float32)
    gate_sig = jax.nn.sigmoid(gate_pre)
    gate_act = gate_pre * gate_sig
    hidden = (gate_act * up_pre).astype(jnp.bfloat16)
    dw_down = jnp.dot(hidden.T, dy_tokens, preferred_element_type=jnp.float32)
    d_hidden = jnp.dot(dy_tokens, w_down.T, preferred_element_type=jnp.float32)
    d_gate = (d_hidden * up_pre * gate_sig * (1.0 + gate_pre * (1.0 - gate_sig))).astype(jnp.bfloat16)
    d_up = (d_hidden * gate_act).astype(jnp.bfloat16)
    dw_gate = jnp.dot(x_tokens.T, d_gate, preferred_element_type=jnp.float32)
    dw_up = jnp.dot(x_tokens.T, d_up, preferred_element_type=jnp.float32)
    dx_sum = (jnp.einsum("hte,dhe->td", dq_f32, w_q.astype(jnp.float32))
              + jnp.einsum("gte,dge->td", dk_sum, w_k.astype(jnp.float32))
              + jnp.einsum("gte,dge->td", dv_sum, w_v.astype(jnp.float32))
              + jnp.dot(d_gate, w_gate.T, preferred_element_type=jnp.float32)
              + jnp.dot(d_up, w_up.T, preferred_element_type=jnp.float32))
    return (dx_sum.astype(jnp.bfloat16), dw_q, dw_k, dw_v, dw_o, dw_gate, dw_up, dw_down)
```

```python
import functools

import jax
import jax.numpy as jnp
from jax import lax
from jax.experimental import pallas as pl
from jax.experimental.pallas import tpu as pltpu
from jax.sharding import PartitionSpec as P

MESH = pl.DeviceIdType.MESH
BF = jnp.bfloat16
F32 = jnp.float32
SUBS = 2


def dot_nt(a, b):
    return lax.dot_general(a, b, (((1,), (1,)), ((), ())), preferred_element_type=F32)


def dot_tn(a, b):
    return lax.dot_general(a, b, (((0,), (0,)), ((), ())), preferred_element_type=F32)


def dot_nn(a, b):
    return jnp.dot(a, b, preferred_element_type=F32)


class Sizes:
    def __init__(self, n_dev, kv_count, tok, d_model, ff, hd):
        self.n, self.kv, self.tok, self.d, self.ff, self.hd = n_dev, kv_count, tok, d_model, ff, hd
        self.chips = n_dev // 2
        self.seq = n_dev * tok
        self.fm = (ff // 128) * 128
        self.ft = ff - self.fm
        assert 0 < 2 * self.ft <= 128 and self.ft % 16 == 0 and hd == 128 and tok == 128
        self.au, self.aq, self.ak, self.av = self.fm, 2 * self.fm, 2 * self.fm + hd, 2 * self.fm + 2 * hd
        self.at = 2 * self.fm + 3 * hd
        self.wa = self.at + 128
        self.yo, self.yt = self.fm, self.fm + hd
        self.wy = self.yt + 128
        self.pair = 2 * tok


def fused_kernel(z_, x_hbm, y_hbm, wq_hbm, wk_hbm, wv_hbm, wo_hbm, wg_hbm, wu_hbm, wd_hbm,
                 dx_out, dwk_out, dwv_out, xo, yo, do, ho,
                 xg, yg, wall, wy, dd, hos, dhs, qs, ks, vs, dka, dva, sc, pb, ds, wqv, wkv, ktmp,
                 dxs, rsend, drecv, rrecv, kvp, kr1, kr2, kr3,
                 wsem, ring_s, sib_s, rsem, lsem, hsem, osem, d_s, d_r, r_s, r_r, k_s, k_r):
    S = z_
    n, chips, tok, pair, d_model, hd = S.n, S.chips, S.tok, S.pair, S.d, S.hd
    sub_rows = tok // SUBS
    scale = hd ** -0.5
    me = lax.axis_index("tp")
    c = lax.rem(me, 2)
    z = lax.div(me, 2)
    step_dir = 1 - 2 * c
    dev = lambda chip: lax.rem(chip + chips, chips) * 2 + c
    nxt, prv = dev(z + step_dir), dev(z - step_dir)
    sib = me + 1 - 2 * c
    a0, a1 = lax.rem(z, 2), lax.rem(lax.div(z, 2), 2)
    part1 = (z + 1 - 2 * a0) * 2 + c
    part2 = (z + 2 - 4 * a1) * 2 + c
    kvi = lax.div(me, n // S.kv)

    barrier = pltpu.get_barrier_semaphore()
    for peer in (sib, nxt, prv, part2):
        pl.semaphore_signal(barrier, inc=1, device_id={"tp": peer}, device_id_type=MESH)

    fm, ft = S.fm, S.ft
    wcopies = [
        pltpu.make_async_copy(wg_hbm.at[pl.ds(0, fm)], wall.at[pl.ds(0, fm)], wsem.at[0]),
        pltpu.make_async_copy(wu_hbm.at[pl.ds(0, fm)], wall.at[pl.ds(S.au, fm)], wsem.at[1]),
        pltpu.make_async_copy(wg_hbm.at[pl.ds(fm, ft)], wall.at[pl.ds(S.at, ft)], wsem.at[2]),
        pltpu.make_async_copy(wu_hbm.at[pl.ds(fm, ft)], wall.at[pl.ds(S.at + ft, ft)], wsem.at[3]),
        pltpu.make_async_copy(wd_hbm.at[pl.ds(0, fm)], wy.at[pl.ds(0, fm)], wsem.at[4]),
        pltpu.make_async_copy(wd_hbm.at[pl.ds(fm, ft)], wy.at[pl.ds(S.yt, ft)], wsem.at[5]),
        pltpu.make_async_copy(wo_hbm, wy.at[pl.ds(S.yo, hd)], wsem.at[6]),
    ]
    qcopy = pltpu.make_async_copy(wq_hbm, wqv, wsem.at[7])
    kcopy = pltpu.make_async_copy(wk_hbm, wkv.at[0], wsem.at[8])
    vcopy = pltpu.make_async_copy(wv_hbm, wkv.at[1], wsem.at[9])
    for cp in [qcopy, kcopy, vcopy] + wcopies:
        cp.start()

    gathered, owned = (xg, yg), (x_hbm, y_hbm)

    def rows(slot, ring, sub):
        return pl.ds(pl.multiple_of(slot * pair + ring * tok + sub * sub_rows, sub_rows), sub_rows)

    def ring_copy(st, slot, sub, src):
        return pltpu.make_async_remote_copy(
            src_ref=src, dst_ref=gathered[st].at[rows(slot + 1, c, sub)],
            send_sem=ring_s.at[st, slot, sub], recv_sem=rsem.at[st, slot + 1, c, sub],
            device_id={"tp": nxt}, device_id_type=MESH)

    def sib_copy(st, slot, sub, src):
        return pltpu.make_async_remote_copy(
            src_ref=src, dst_ref=gathered[st].at[rows(slot, c, sub)],
            send_sem=sib_s.at[st, slot, sub], recv_sem=rsem.at[st, slot, c, sub],
            device_id={"tp": sib}, device_id_type=MESH)

    def own_src(st, sub):
        return owned[st].at[pl.ds(sub * sub_rows, sub_rows)]

    def here(st, slot, sub):
        return gathered[st].at[rows(slot, c, sub)]

    def wait_block(st, slot, ring, sub):
        ref = gathered[st].at[rows(slot, ring, sub)]
        pltpu.make_async_remote_copy(
            src_ref=ref, dst_ref=ref, send_sem=ring_s.at[st, 0, sub], recv_sem=rsem.at[st, slot, ring, sub],
            device_id={"tp": sib}, device_id_type=MESH).wait_recv()

    def start_own(st):
        for sub in range(SUBS):
            ring_copy(st, 0, sub, own_src(st, sub)).start()
            sib_copy(st, 0, sub, own_src(st, sub)).start()

    def pump(st, slot, sub):
        wait_block(st, slot, c, sub)

        @pl.when(slot < chips - 1)
        def _():
            ring_copy(st, slot, sub, here(st, slot, sub)).start()
        sib_copy(st, slot, sub, here(st, slot, sub)).start()

    local = [pltpu.make_async_copy(owned[st], gathered[st].at[pl.ds(pl.multiple_of(c * tok, tok), tok)], lsem.at[st])
             for st in range(2)]
    for cp in local:
        cp.start()
    pl.semaphore_wait(barrier, 4)
    start_own(0)

    wall[S.at + 2 * ft:S.wa, :] = jnp.zeros((128 - 2 * ft, d_model), BF)
    wy[S.yt + ft:S.wy, :] = jnp.zeros((128 - ft, d_model), BF)
    dka[...] = jnp.zeros_like(dka)
    dva[...] = jnp.zeros_like(dva)
    qcopy.wait()
    kcopy.wait()
    vcopy.wait()
    span = 256

    @pl.loop(0, d_model // span)
    def _(i):
        r0 = pl.multiple_of(i * span, span)
        wall[S.aq:S.aq + hd, pl.ds(r0, span)] = wqv[pl.ds(r0, span), :].T
        for w in range(2):
            ktmp[...] = wkv[w, pl.ds(r0, span)].reshape(S.kv * span, hd).astype(F32)
            one = ktmp[pl.ds(kvi, span, stride=S.kv), :]
            off = S.ak + w * hd
            wall[off:off + hd, pl.ds(r0, span)] = one.T.astype(BF)
    for cp in wcopies:
        cp.wait()
    for cp in local:
        cp.wait()

    def block_of(slot, ring):
        chip = lax.rem(z + chips + jnp.where(ring == 0, -slot, slot), chips)
        return chip * 2 + ring

    def slot_rows(slot):
        return pl.ds(pl.multiple_of(slot * pair, pair), pair)

    cut = 1024

    def fwd_first(slot):
        out = dot_nt(xg[slot_rows(slot), :], wall[0:cut, :])
        dd[slot_rows(slot), 0:cut] = out.astype(BF)

    def fwd_second(slot):
        out = dot_nt(xg[slot_rows(slot), :], wall[cut:S.wa, :]).astype(BF)
        dd[slot_rows(slot), cut:S.wa] = out
        for ring in range(2):
            tgt = pl.ds(pl.multiple_of(block_of(slot, ring) * tok, tok), tok)
            part = out[ring * tok:(ring + 1) * tok]
            qs[tgt, :] = part[:, S.aq - cut:S.ak - cut]
            ks[tgt, :] = part[:, S.ak - cut:S.av - cut]
            vs[tgt, :] = part[:, S.av - cut:S.at - cut]

    @pl.loop(1, chips + 1)
    def _(it):
        @pl.when(it < chips)
        def _():
            pump(0, it, 0)
        for sub in range(SUBS):
            wait_block(0, it - 1, 1 - c, sub)
        fwd_first(it - 1)

        @pl.when(it < chips)
        def _():
            pump(0, it, 1)

        @pl.when(it == chips - 2)
        def _():
            start_own(1)
        fwd_second(it - 1)

    xcopy = pltpu.make_async_copy(xg, xo, osem.at[0])
    xcopy.start()

    def h_copy(slot):
        return pltpu.make_async_copy(hos.at[lax.rem(slot, 2)], ho.at[slot_rows(slot)], hsem.at[lax.rem(slot, 2)])

    lane = lax.broadcasted_iota(jnp.int32, (32, 128), 1)

    def mlp_mid(slot):
        buf = lax.rem(slot, 2)

        @pl.loop(0, pair // 32)
        def _(i):
            r = pl.ds(pl.multiple_of(slot * pair + i * 32, 32), 32)
            rl = pl.ds(pl.multiple_of(i * 32, 32), 32)

            def grads(a, u, dh):
                sg = jax.nn.sigmoid(a)
                act = a * sg
                return act * u, dh * u * sg * (1.0 + a * (1.0 - sg)), dh * act

            for j in range(0, fm, 128):
                h, da, du = grads(dd[r, j:j + 128].astype(F32), dd[r, S.au + j:S.au + j + 128].astype(F32), dhs[rl, j:j + 128])
                hos[buf, rl, j:j + 128] = h.astype(BF)
                dd[r, j:j + 128] = da.astype(BF)
                dd[r, S.au + j:S.au + j + 128] = du.astype(BF)
            both = dd[r, S.at:S.wa].astype(F32)
            h, da, du = grads(both, pltpu.roll(both, 128 - ft, 1), dhs[rl, S.yt:S.wy])
            hos[buf, rl, S.yt:S.wy] = h.astype(BF)
            rest = jnp.where(lane < ft, da, jnp.where(lane < 2 * ft, pltpu.roll(du, ft, 1), 0.0))
            dd[r, S.at:S.wa] = rest.astype(BF)

    kc = 256

    def attend(slot, ring, blk, chunks):
        rl = pl.ds(pl.multiple_of(ring * tok, tok), tok)
        qrow = pl.ds(pl.multiple_of(blk * tok, tok), tok)
        q = qs[qrow, :]
        dout = dhs[rl, S.yo:S.yt].astype(BF)
        run = None
        for ch in range(chunks):
            s = dot_nt(q, ks[ch * kc:(ch + 1) * kc, :]) * scale
            if ch >= chunks - 2:
                col = lax.broadcasted_iota(jnp.int32, (tok, kc), 1) + ch * kc
                row = lax.broadcasted_iota(jnp.int32, (tok, kc), 0) + blk * tok
                s = jnp.where(col <= row, s, -jnp.inf)
            sc[:, ch * kc:(ch + 1) * kc] = s
            top = jnp.maximum(s[:, 0:128], s[:, 128:256])
            run = top if run is None else jnp.maximum(run, top)
        m = jnp.max(run, axis=1, keepdims=True)
        tot = jnp.zeros((tok, 128), F32)
        for ch in range(chunks):
            p = jnp.exp(sc[:, ch * kc:(ch + 1) * kc] - m)
            sc[:, ch * kc:(ch + 1) * kc] = p
            tot = tot + p[:, 0:128] + p[:, 128:256]
        inv = 1.0 / jnp.sum(tot, axis=1, keepdims=True)
        for ch in range(chunks):
            p = sc[:, ch * kc:(ch + 1) * kc] * inv
            sc[:, ch * kc:(ch + 1) * kc] = p
            pb[:, ch * kc:(ch + 1) * kc] = p.astype(BF)
        length = chunks * kc
        o = dot_nn(pb[:, 0:length], vs[0:length, :]).astype(BF)
        hos[lax.rem(slot, 2), rl, S.yo:S.yt] = o
        delta = jnp.sum(dout.astype(F32) * o.astype(F32), axis=1, keepdims=True)
        for ch in range(chunks):
            dp = dot_nt(dout, vs[ch * kc:(ch + 1) * kc, :])
            ds[:, ch * kc:(ch + 1) * kc] = (sc[:, ch * kc:(ch + 1) * kc] * (dp - delta)).astype(BF)
        dq = dot_nn(ds[:, 0:length], ks[0:length, :]) * scale
        dd[pl.ds(pl.multiple_of(slot * pair + ring * tok, tok), tok), S.aq:S.ak] = dq.astype(BF)
        for ch in range(chunks):
            dka[ch * kc:(ch + 1) * kc, :] += dot_tn(ds[:, ch * kc:(ch + 1) * kc], q)
            dva[ch * kc:(ch + 1) * kc, :] += dot_tn(pb[:, ch * kc:(ch + 1) * kc], dout)

    @pl.loop(1, chips + 1)
    def _(it):
        slot = it - 1

        @pl.when(it < chips)
        def _():
            pump(1, it, 0)
        for sub in range(SUBS):
            wait_block(1, slot, 1 - c, sub)
        dhs[...] = dot_nt(yg[slot_rows(slot), :], wy[...])

        @pl.when(it < chips)
        def _():
            pump(1, it, 1)

        @pl.when(slot >= 2)
        def _():
            h_copy(slot - 2).wait()
        mlp_mid(slot)

        @pl.loop(0, 2)
        def _(ring):
            blk = block_of(slot, ring)
            group = lax.div(blk, 4)
            for v in range(n // 4):
                @pl.when(group == v)
                def _():
                    attend(slot, ring, blk, 2 * (v + 1))
        h_copy(slot).start()

    ycopy = pltpu.make_async_copy(yg, yo, osem.at[1])
    ycopy.start()

    @pl.loop(0, chips)
    def _(slot):
        for ring in range(2):
            src = pl.ds(pl.multiple_of(block_of(slot, ring) * tok, tok), tok)
            dst = pl.ds(pl.multiple_of(slot * pair + ring * tok, tok), tok)
            dd[dst, S.ak:S.av] = (dka[src, :] * scale).astype(BF)
            dd[dst, S.av:S.at] = dva[src, :].astype(BF)

    dcopy = pltpu.make_async_copy(dd, do, osem.at[2])
    dcopy.start()

    def slot_at(k):
        return lax.rem(k + 1, chips)

    def mine(ref, k):
        return ref.at[lax.rem(k, 2), pl.ds(pl.multiple_of(c * tok, tok), tok)]

    def d_copy(k):
        return pltpu.make_async_remote_copy(
            src_ref=dxs.at[lax.rem(k, 2), pl.ds(pl.multiple_of((1 - c) * tok, tok), tok)], dst_ref=drecv.at[k],
            send_sem=d_s.at[k], recv_sem=d_r.at[k], device_id={"tp": sib}, device_id_type=MESH)

    def r_copy(k, sub):
        cut_rows = pl.ds(sub * sub_rows, sub_rows)
        return pltpu.make_async_remote_copy(
            src_ref=rsend.at[lax.rem(k, 2), cut_rows], dst_ref=rrecv.at[k + 1, cut_rows],
            send_sem=r_s.at[k, sub], recv_sem=r_r.at[k + 1, sub], device_id={"tp": nxt}, device_id_type=MESH)

    def dx_part(k):
        slot = slot_at(k)
        buf = lax.rem(k, 2)
        lhs = dd[slot_rows(slot), :]
        for nb in range(0, d_model, 512):
            dxs[buf, :, nb:nb + 512] = dot_nn(lhs, wall[:, nb:nb + 512]).astype(BF)
        d_copy(k).start()

    def dx_pump(k, sub):
        cut_rows = pl.ds(sub * sub_rows, sub_rows)
        mine_rows = pl.ds(pl.multiple_of(c * tok + sub * sub_rows, sub_rows), sub_rows)

        @pl.when(k > 0)
        def _():
            rref = rrecv.at[k, cut_rows]
            pltpu.make_async_remote_copy(
                src_ref=rref, dst_ref=rref, send_sem=r_s.at[0, sub], recv_sem=r_r.at[k, sub],
                device_id={"tp": nxt}, device_id_type=MESH).wait_recv()

        @pl.when(jnp.logical_and(k >= 2, k < chips - 1))
        def _():
            r_copy(k - 2, sub).wait_send()
        base = dxs[lax.rem(k, 2), mine_rows, :].astype(F32) + drecv[k, cut_rows, :].astype(F32)

        @pl.when(k == 0)
        def _():
            rsend[0, cut_rows, :] = base.astype(BF)

        @pl.when(jnp.logical_and(k > 0, k < chips - 1))
        def _():
            rsend[lax.rem(k, 2), cut_rows, :] = (base + rrecv[k, cut_rows, :].astype(F32)).astype(BF)

        @pl.when(k == chips - 1)
        def _():
            dx_out[cut_rows, :] = (base + rrecv[k, cut_rows, :].astype(F32)).astype(BF)

        @pl.when(k < chips - 1)
        def _():
            r_copy(k, sub).start()

    k1 = pltpu.make_async_remote_copy(src_ref=kvp.at[1 - c], dst_ref=kr1, send_sem=k_s.at[0], recv_sem=k_r.at[0],
                                      device_id={"tp": sib}, device_id_type=MESH)
    k2 = pltpu.make_async_remote_copy(src_ref=kvp.at[c, 1 - a0], dst_ref=kr2, send_sem=k_s.at[1], recv_sem=k_r.at[1],
                                      device_id={"tp": part1}, device_id_type=MESH)
    k3 = pltpu.make_async_remote_copy(src_ref=kvp.at[c, a0, 1 - a1], dst_ref=kr3, send_sem=k_s.at[2], recv_sem=k_r.at[2],
                                      device_id={"tp": part2}, device_id_type=MESH)

    def kv_start():
        lhs = dd[:, S.ak:S.at]
        for e in range(n // S.kv):
            out = dot_tn(lhs, xg[:, e * kc:(e + 1) * kc])
            kvp[e % 2, (e // 2) % 2, e // 4] = out
        k1.start()

    def kv_second():
        k1.wait_recv()
        kvp[c] = kvp[c] + kr1[...]
        k2.start()

    def kv_third():
        k2.wait_recv()
        kvp[c, a0] = kvp[c, a0] + kr2[...]
        k3.start()

    def kv_last():
        k3.wait_recv()
        fin = kvp[c, a0, a1] + kr3[...]
        dwk_out[0] = fin[0:hd].T
        dwv_out[0] = fin[hd:2 * hd].T

    dx_part(0)

    @pl.loop(0, chips)
    def _(k):
        dref = drecv.at[k]
        pltpu.make_async_remote_copy(
            src_ref=dref, dst_ref=dref, send_sem=d_s.at[0], recv_sem=d_r.at[k],
            device_id={"tp": sib}, device_id_type=MESH).wait_recv()
        dx_pump(k, 0)

        @pl.when(jnp.logical_and(k >= 1, k < chips - 1))
        def _():
            d_copy(k - 1).wait_send()

        @pl.when(k < chips - 1)
        def _():
            dx_part(k + 1)
        dx_pump(k, 1)

        @pl.when(k == 0)
        def _():
            kv_start()

        @pl.when(k == 1)
        def _():
            kv_second()

        @pl.when(k == 4)
        def _():
            kv_third()

    kv_last()

    for cp in (k1, k2, k3):
        cp.wait_send()
    for sub in range(SUBS):
        for k in range(chips - 3, chips - 1):
            r_copy(k, sub).wait_send()
    for k in range(chips - 2, chips):
        d_copy(k).wait_send()

    @pl.loop(0, chips)
    def _(slot):
        for st in range(2):
            for sub in range(SUBS):
                @pl.when(slot < chips - 1)
                def _():
                    ring_copy(st, slot, sub, here(st, slot, sub)).wait_send()
                sib_copy(st, slot, sub, here(st, slot, sub)).wait_send()
    for slot in range(chips - 2, chips):
        h_copy(slot).wait()
    xcopy.wait()
    ycopy.wait()
    dcopy.wait()


def weights_kernel(z_, x_ref, y_ref, d_ref, h_ref, wg_out, wu_out, wd_out, wq_out, wo_out):
    S = z_
    fm, ft, hd = S.fm, S.ft, S.hd
    x, y = x_ref[...], y_ref[...]
    wg_out[0:fm, :] = dot_tn(d_ref[:, 0:fm], x)
    wu_out[0:fm, :] = dot_tn(d_ref[:, S.au:S.au + fm], x)
    wq_out[...] = dot_tn(d_ref[:, S.aq:S.ak], x).T
    rest = dot_tn(d_ref[:, S.at:S.wa], x)
    wg_out[fm:fm + ft, :] = rest[0:ft]
    wu_out[fm:fm + ft, :] = rest[ft:2 * ft]
    wd_out[0:fm, :] = dot_tn(h_ref[:, 0:fm], y)
    rest = dot_tn(h_ref[:, S.yo:S.wy], y)
    wo_out[...] = rest[0:hd]
    wd_out[fm:fm + ft, :] = rest[hd:hd + ft]


def solution(mesh):
    n_dev = mesh.shape["tp"]

    def local_step(x_loc, dy_loc, w_q, w_k, w_v, w_o, w_gate, w_up, w_down):
        tok, d_model = x_loc.shape
        ff, hd, kv = w_gate.shape[1], w_q.shape[2], w_k.shape[1]
        S = Sizes(n_dev, kv, tok, d_model, ff, hd)
        seq, chips, pair = S.seq, S.chips, S.pair
        any_spec = pl.BlockSpec(memory_space=pl.ANY)
        vm = pl.BlockSpec(memory_space=pltpu.VMEM)
        dma = pltpu.SemaphoreType.DMA
        reps = n_dev // kv
        dcut = d_model // reps
        outs = pl.pallas_call(
            functools.partial(fused_kernel, S),
            out_shape=(
                jax.ShapeDtypeStruct((tok, d_model), BF),
                jax.ShapeDtypeStruct((1, dcut, hd), F32),
                jax.ShapeDtypeStruct((1, dcut, hd), F32),
                jax.ShapeDtypeStruct((seq, d_model), BF),
                jax.ShapeDtypeStruct((seq, d_model), BF),
                jax.ShapeDtypeStruct((seq, S.wa), BF),
                jax.ShapeDtypeStruct((seq, S.wy), BF),
            ),
            in_specs=[any_spec] * 9,
            out_specs=(vm, vm, vm) + (any_spec,) * 4,
            scratch_shapes=[
                pltpu.VMEM((seq, d_model), BF), pltpu.VMEM((seq, d_model), BF),
                pltpu.VMEM((S.wa, d_model), BF), pltpu.VMEM((S.wy, d_model), BF),
                pltpu.VMEM((seq, S.wa), BF), pltpu.VMEM((2, pair, S.wy), BF), pltpu.VMEM((pair, S.wy), F32),
                pltpu.VMEM((seq, hd), BF), pltpu.VMEM((seq, hd), BF), pltpu.VMEM((seq, hd), BF),
                pltpu.VMEM((seq, hd), F32), pltpu.VMEM((seq, hd), F32),
                pltpu.VMEM((tok, seq), F32), pltpu.VMEM((tok, seq), BF), pltpu.VMEM((tok, seq), BF),
                pltpu.VMEM((d_model, hd), BF), pltpu.VMEM((2, d_model, kv, hd), BF), pltpu.VMEM((kv * 256, hd), F32),
                pltpu.VMEM((2, pair, d_model), BF), pltpu.VMEM((2, tok, d_model), BF),
                pltpu.VMEM((chips, tok, d_model), BF), pltpu.VMEM((chips, tok, d_model), BF),
                pltpu.VMEM((2, 2, reps // 4, 2 * hd, dcut), F32), pltpu.VMEM((2, reps // 4, 2 * hd, dcut), F32),
                pltpu.VMEM((reps // 4, 2 * hd, dcut), F32), pltpu.VMEM((2 * hd, dcut), F32),
                dma((10,)), dma((2, chips, SUBS)), dma((2, chips, SUBS)), dma((2, chips, 2, SUBS)), dma((2,)), dma((2,)),
                dma((3,)), dma((chips,)), dma((chips,)), dma((chips, SUBS)), dma((chips, SUBS)), dma((3,)), dma((3,)),
            ],
            compiler_params=pltpu.CompilerParams(collective_id=0, has_side_effects=True, vmem_limit_bytes=67043328),
            name="fused",
        )(x_loc, dy_loc, w_q[:, 0, :], w_k, w_v, w_o[0], w_gate.T, w_up.T, w_down)
        dx, dwk, dwv, xo, yo, do, ho = outs
        nb = 256
        col = lambda i: (0, i)
        fixed = lambda i: (0, 0)
        wg, wu, wd, wq, wo = pl.pallas_call(
            functools.partial(weights_kernel, S),
            grid=(d_model // nb,),
            in_specs=[pl.BlockSpec((seq, nb), col), pl.BlockSpec((seq, nb), col),
                      pl.BlockSpec((seq, S.wa), fixed), pl.BlockSpec((seq, S.wy), fixed)],
            out_specs=[pl.BlockSpec((ff, nb), col), pl.BlockSpec((ff, nb), col), pl.BlockSpec((ff, nb), col),
                       pl.BlockSpec((nb, hd), lambda i: (i, 0)), pl.BlockSpec((hd, nb), col)],
            out_shape=(jax.ShapeDtypeStruct((ff, d_model), F32), jax.ShapeDtypeStruct((ff, d_model), F32),
                       jax.ShapeDtypeStruct((ff, d_model), F32), jax.ShapeDtypeStruct((d_model, hd), F32),
                       jax.ShapeDtypeStruct((hd, d_model), F32)),
            compiler_params=pltpu.CompilerParams(vmem_limit_bytes=60 << 20),
            name="weights",
        )(xo, yo, do, ho)
        return (dx, wq.reshape(d_model, 1, hd), dwk, dwv, wo[None], wg.T, wu.T, wd)

    token_spec = P(("dp", "tp"), None)
    in_specs = (token_spec, token_spec, P(None, "tp", None), P(None, None, None), P(None, None, None),
                P("tp", None, None), P(None, "tp"), P(None, "tp"), P("tp", None))
    out_specs = (token_spec, P("dp", "tp", None), P(("dp", "tp"), None, None), P(("dp", "tp"), None, None),
                 P(("dp", "tp"), None, None), P("dp", "tp"), P("dp", "tp"), P(("dp", "tp"), None))
    return jax.shard_map(local_step, mesh=mesh, in_specs=in_specs, out_specs=out_specs, check_vma=False)
```

```python
import functools

import jax
import jax.numpy as jnp
from jax import lax
from jax.experimental import pallas as pl
from jax.experimental.pallas import tpu as pltpu
from jax.sharding import PartitionSpec as P

MESH = pl.DeviceIdType.MESH
BF = jnp.bfloat16
F32 = jnp.float32
SUBS = 2
KV_PARTS, KV_LAG = 8, 2


def dot_nt(a, b):
    return lax.dot_general(a, b, (((1,), (1,)), ((), ())), preferred_element_type=F32)


def dot_tn(a, b):
    return lax.dot_general(a, b, (((0,), (0,)), ((), ())), preferred_element_type=F32)


def dot_nn(a, b):
    return jnp.dot(a, b, preferred_element_type=F32)


class Sizes:
    def __init__(self, n_dev, kv_count, tok, d_model, ff, hd):
        self.n, self.kv, self.tok, self.d, self.ff, self.hd = n_dev, kv_count, tok, d_model, ff, hd
        self.chips = n_dev // 2
        self.seq = n_dev * tok
        self.fm = (ff // 128) * 128
        self.ft = ff - self.fm
        assert 0 < 2 * self.ft <= 128 and self.ft % 16 == 0 and hd == 128 and tok == 128
        self.au, self.aq, self.at = self.fm, 2 * self.fm, 2 * self.fm + hd
        self.ak = self.at + 128
        self.av, self.wa = self.ak + hd, self.ak + 2 * hd
        self.yt, self.yo = self.fm, self.fm + 128
        self.wy = self.yo + hd
        self.pair = 2 * tok


def fused_kernel(z_, x_hbm, y_hbm, wq_hbm, wk_hbm, wv_hbm, wo_hbm, wg_hbm, wu_hbm, wd_hbm,
                 dx_own, dx_send, dwk_out, dwv_out, wg_out, wu_out, wq_out, wd_out, wo_out,
                 xg, yg, wall, wy, dd, hh, dhs, dob, qs, ks, vs, pb, ds, wqv, wkv, ktmp,
                 dxs, rsend, drecv, rrecv, kvd, kvl, kvr, kvf, kvg, stage,
                 wsem, ring_s, sib_s, rsem, lsem, gsem, d_s, d_r, r_s, r_r, k_s, k_r, line_s, line_r):
    S = z_
    n, chips, tok, pair, d_model, hd = S.n, S.chips, S.tok, S.pair, S.d, S.hd
    sub_rows = tok // SUBS
    scale = hd ** -0.5
    me = lax.axis_index("tp")
    c = lax.rem(me, 2)
    z = lax.div(me, 2)
    step_dir = 1 - 2 * c
    dev = lambda chip: lax.rem(chip + chips, chips) * 2 + c
    nxt, prv = dev(z + step_dir), dev(z - step_dir)
    sib = me + 1 - 2 * c
    kvi = lax.div(me, n // S.kv)

    barrier = pltpu.get_barrier_semaphore()
    for peer in (sib, nxt, prv):
        pl.semaphore_signal(barrier, inc=1, device_id={"tp": peer}, device_id_type=MESH)

    fm, ft = S.fm, S.ft
    wcopies = [
        pltpu.make_async_copy(wg_hbm.at[pl.ds(0, fm)], wall.at[pl.ds(0, fm)], wsem.at[0]),
        pltpu.make_async_copy(wu_hbm.at[pl.ds(0, fm)], wall.at[pl.ds(S.au, fm)], wsem.at[1]),
        pltpu.make_async_copy(wg_hbm.at[pl.ds(fm, ft)], wall.at[pl.ds(S.at, ft)], wsem.at[2]),
        pltpu.make_async_copy(wu_hbm.at[pl.ds(fm, ft)], wall.at[pl.ds(S.at + ft, ft)], wsem.at[3]),
        pltpu.make_async_copy(wd_hbm.at[pl.ds(0, fm)], wy.at[pl.ds(0, fm)], wsem.at[4]),
        pltpu.make_async_copy(wd_hbm.at[pl.ds(fm, ft)], wy.at[pl.ds(S.yt, ft)], wsem.at[5]),
        pltpu.make_async_copy(wo_hbm, wy.at[pl.ds(S.yo, hd)], wsem.at[6]),
    ]
    qcopy = pltpu.make_async_copy(wq_hbm, wqv, wsem.at[7])
    kcopy = pltpu.make_async_copy(wk_hbm, wkv.at[0], wsem.at[8])
    vcopy = pltpu.make_async_copy(wv_hbm, wkv.at[1], wsem.at[9])
    gathered, owned = (xg, yg), (x_hbm, y_hbm)
    local = [pltpu.make_async_copy(owned[st], gathered[st].at[pl.ds(pl.multiple_of(c * tok, tok), tok)], lsem.at[st])
             for st in range(2)]
    for cp in local + [qcopy, kcopy, vcopy]:
        cp.start()

    def rows(slot, ring, sub):
        return pl.ds(pl.multiple_of(slot * pair + ring * tok + sub * sub_rows, sub_rows), sub_rows)

    def ring_copy(st, slot, sub, src):
        return pltpu.make_async_remote_copy(
            src_ref=src, dst_ref=gathered[st].at[rows(slot + 1, c, sub)],
            send_sem=ring_s.at[st, slot, sub], recv_sem=rsem.at[st, slot + 1, c, sub],
            device_id={"tp": nxt}, device_id_type=MESH)

    def sib_copy(st, slot, sub, src):
        return pltpu.make_async_remote_copy(
            src_ref=src, dst_ref=gathered[st].at[rows(slot, c, sub)],
            send_sem=sib_s.at[st, slot, sub], recv_sem=rsem.at[st, slot, c, sub],
            device_id={"tp": sib}, device_id_type=MESH)

    def here(st, slot, sub):
        return gathered[st].at[rows(slot, c, sub)]

    def wait_block(st, slot, ring, sub):
        ref = gathered[st].at[rows(slot, ring, sub)]
        pltpu.make_async_remote_copy(
            src_ref=ref, dst_ref=ref, send_sem=ring_s.at[st, 0, sub], recv_sem=rsem.at[st, slot, ring, sub],
            device_id={"tp": sib}, device_id_type=MESH).wait_recv()

    def start_ring(st):
        for sub in range(SUBS):
            ring_copy(st, 0, sub, here(st, 0, sub)).start()

    def start_sib(st):
        for sub in range(SUBS):
            sib_copy(st, 0, sub, here(st, 0, sub)).start()

    def pump(st, slot, sub):
        wait_block(st, slot, c, sub)

        @pl.when(slot < chips - 1)
        def _():
            ring_copy(st, slot, sub, here(st, slot, sub)).start()
        sib_copy(st, slot, sub, here(st, slot, sub)).start()

    pl.semaphore_wait(barrier, 3)
    local[0].wait()
    start_ring(0)
    local[1].wait()
    for st in range(2):
        start_sib(st)
    for cp in wcopies:
        cp.start()

    wall[S.at + 2 * ft:S.ak, :] = jnp.zeros((128 - 2 * ft, d_model), BF)
    wy[S.yt + ft:S.yo, :] = jnp.zeros((128 - ft, d_model), BF)
    for i in (1, 2):
        stage[i] = jnp.zeros(stage.shape[1:], F32)
    rrecv[0] = jnp.zeros(rrecv.shape[1:], BF)
    qcopy.wait()
    kcopy.wait()
    vcopy.wait()
    span = 256

    @pl.loop(0, d_model // span)
    def _(i):
        r0 = pl.multiple_of(i * span, span)
        wall[S.aq:S.aq + hd, pl.ds(r0, span)] = wqv[pl.ds(r0, span), :].T
        for w in range(2):
            ktmp[...] = wkv[w, pl.ds(r0, span)].reshape(S.kv * span, hd).astype(F32)
            one = ktmp[pl.ds(kvi, span, stride=S.kv), :]
            off = S.ak + w * hd
            wall[off:off + hd, pl.ds(r0, span)] = one.T.astype(BF)
    pump(0, 1, 0)
    for cp in wcopies:
        cp.wait()

    def block_of(slot, ring):
        chip = lax.rem(z + chips + jnp.where(ring == 0, -slot, slot), chips)
        return chip * 2 + ring

    def slot_rows(slot):
        return pl.ds(pl.multiple_of(slot * pair, pair), pair)

    cut = 1024

    def fwd_first(slot):
        out = dot_nt(xg[slot_rows(slot), :], wall[0:cut, :])
        dd[slot_rows(slot), 0:cut] = out.astype(BF)

    def fwd_second(slot):
        out = dot_nt(xg[slot_rows(slot), :], wall[cut:S.wa, :]).astype(BF)
        dd[slot_rows(slot), cut:S.wa] = out
        for ring in range(2):
            tgt = pl.ds(pl.multiple_of(block_of(slot, ring) * tok, tok), tok)
            part = out[ring * tok:(ring + 1) * tok]
            qs[tgt, :] = part[:, S.aq - cut:S.at - cut]
            ks[tgt, :] = part[:, S.ak - cut:S.av - cut]
            vs[tgt, :] = part[:, S.av - cut:S.wa - cut]

    lane = lax.broadcasted_iota(jnp.int32, (32, 128), 1)

    def mlp_mid(slot):
        @pl.loop(0, pair // 32)
        def _(i):
            r = pl.ds(pl.multiple_of(slot * pair + i * 32, 32), 32)
            rl = pl.ds(pl.multiple_of(i * 32, 32), 32)

            def grads(a, u, dh):
                sg = jax.nn.sigmoid(a)
                act = a * sg
                return act * u, dh * u * sg * (1.0 + a * (1.0 - sg)), dh * act

            for j in range(0, fm, 128):
                h, da, du = grads(dd[r, j:j + 128].astype(F32), dd[r, S.au + j:S.au + j + 128].astype(F32), dhs[rl, j:j + 128])
                hh[r, j:j + 128] = h.astype(BF)
                dd[r, j:j + 128] = da.astype(BF)
                dd[r, S.au + j:S.au + j + 128] = du.astype(BF)
            both = dd[r, S.at:S.ak].astype(F32)
            h, da, du = grads(both, pltpu.roll(both, 128 - ft, 1), dhs[rl, fm:fm + 128])
            hh[r, S.yt:S.yo] = h.astype(BF)
            rest = jnp.where(lane < ft, da, jnp.where(lane < 2 * ft, pltpu.roll(du, ft, 1), 0.0))
            dd[r, S.at:S.ak] = rest.astype(BF)

    def y_out(slot, ring):
        part = pl.ds(pl.multiple_of(slot * pair + ring * tok, tok), tok)
        dob[...] = dot_nt(yg[part, :], wy[S.yo:S.wy, :]).astype(BF)

    def y_first(slot):
        dhs[...] = dot_nt(yg[slot_rows(slot), :], wy[0:S.yo, :])

    for sub in range(SUBS):
        wait_block(1, 0, 1 - c, sub)
    y_first(0)

    @pl.loop(0, chips)
    def _(slot):
        for sub in range(SUBS):
            wait_block(0, slot, 1 - c, sub)
        fwd_first(slot)

        @pl.when(slot < chips - 1)
        def _():
            pump(0, slot + 1, 1)

        @pl.when(slot == chips - 3)
        def _():
            start_ring(1)

        @pl.when(slot == chips - 1)
        def _():
            pump(1, 1, 0)
        fwd_second(slot)

        @pl.when(slot == 0)
        def _():
            mlp_mid(0)

        @pl.when(slot < chips - 2)
        def _():
            pump(0, slot + 2, 0)

    kc = 256
    sc, dka, dva = stage.at[0], stage.at[1], stage.at[2]

    def attend(slot, ring, blk, chunks):
        qrow = pl.ds(pl.multiple_of(blk * tok, tok), tok)
        q = qs[qrow, :]
        dout = dob[...]
        srow = pl.ds(pl.multiple_of(slot * pair + ring * tok, tok), tok)
        run = None
        for ch in range(chunks):
            s = dot_nt(q, ks[ch * kc:(ch + 1) * kc, :]) * scale
            if ch >= chunks - 2:
                col = lax.broadcasted_iota(jnp.int32, (tok, kc), 1) + ch * kc
                row = lax.broadcasted_iota(jnp.int32, (tok, kc), 0) + blk * tok
                s = jnp.where(col <= row, s, -jnp.inf)
            sc[:, ch * kc:(ch + 1) * kc] = s
            top = jnp.maximum(s[:, 0:128], s[:, 128:256])
            run = top if run is None else jnp.maximum(run, top)
        m = jnp.max(run, axis=1, keepdims=True)
        tot = jnp.zeros((tok, 128), F32)
        for ch in range(chunks):
            p = jnp.exp(sc[:, ch * kc:(ch + 1) * kc] - m)
            sc[:, ch * kc:(ch + 1) * kc] = p
            tot = tot + p[:, 0:128] + p[:, 128:256]
        inv = 1.0 / jnp.sum(tot, axis=1, keepdims=True)
        for ch in range(chunks):
            p = sc[:, ch * kc:(ch + 1) * kc] * inv
            sc[:, ch * kc:(ch + 1) * kc] = p
            pb[:, ch * kc:(ch + 1) * kc] = p.astype(BF)
        length = chunks * kc
        o = dot_nn(pb[:, 0:length], vs[0:length, :]).astype(BF)
        hh[srow, S.yo:S.wy] = o
        delta = jnp.sum(dout.astype(F32) * o.astype(F32), axis=1, keepdims=True)
        for ch in range(chunks):
            dp = dot_nt(dout, vs[ch * kc:(ch + 1) * kc, :])
            ds[:, ch * kc:(ch + 1) * kc] = (sc[:, ch * kc:(ch + 1) * kc] * (dp - delta)).astype(BF)
        dq = dot_nn(ds[:, 0:length], ks[0:length, :]) * scale
        dd[srow, S.aq:S.at] = dq.astype(BF)
        for ch in range(chunks):
            for acc, lhs, rhs in ((dka, ds, q), (dva, pb, dout)):
                acc[:, ch * kc:(ch + 1) * kc] += dot_tn(rhs, lhs[:, ch * kc:(ch + 1) * kc])

    def attend_ring(slot, ring):
        blk = block_of(slot, ring)
        group = lax.div(blk, 4)
        for v in range(n // 4):
            @pl.when(group == v)
            def _():
                attend(slot, ring, blk, 2 * (v + 1))

    first_core = c == 0
    kv_in = pltpu.make_async_remote_copy(src_ref=ks, dst_ref=kvd, send_sem=k_s.at[0], recv_sem=k_r.at[0],
                                         device_id={"tp": sib}, device_id_type=MESH)

    def kv_own():
        for slot in range(chips):
            for ring in range(2):
                at = pl.multiple_of(block_of(slot, ring) * tok, tok)
                dst = slice(slot * pair + ring * tok, slot * pair + (ring + 1) * tok)
                dk = (dka[:, pl.ds(at, tok)] * scale).astype(BF).T
                dv = dva[:, pl.ds(at, tok)].astype(BF).T
                dd[dst, S.ak:S.av] = dk
                dd[dst, S.av:S.wa] = dv
                qs[pl.ds(at, tok), :] = jnp.where(first_core, dk, dv)
                ks[pl.ds(at, tok), :] = jnp.where(first_core, dv, dk)
        kv_in.start()

    def d_copy(k):
        return pltpu.make_async_remote_copy(
            src_ref=dxs.at[lax.rem(k, 2), pl.ds(pl.multiple_of((1 - c) * tok, tok), tok)], dst_ref=drecv.at[k],
            send_sem=d_s.at[k], recv_sem=d_r.at[k], device_id={"tp": sib}, device_id_type=MESH)

    def dx_part(k):
        buf = lax.rem(k, 2)
        lhs = dd[slot_rows(lax.rem(k + 1, chips)), :]
        for nb in range(0, d_model, 512):
            dxs[buf, :, nb:nb + 512] = dot_nn(lhs, wall[:, nb:nb + 512]).astype(BF)
        d_copy(k).start()

    @pl.loop(0, chips)
    def _(slot):
        y_out(slot, c)
        attend_ring(slot, c)

        @pl.when(jnp.logical_and(slot > 0, slot < chips - 1))
        def _():
            pump(1, slot + 1, 0)

        @pl.when(slot > 0)
        def _():
            for sub in range(SUBS):
                wait_block(1, slot, 1 - c, sub)
        y_out(slot, 1 - c)
        attend_ring(slot, 1 - c)

        @pl.when(slot == chips - 1)
        def _():
            kv_own()
            dx_part(jnp.int32(0))

        @pl.when(slot > 0)
        def _():
            y_first(slot)
            mlp_mid(slot)

        @pl.when(slot < chips - 1)
        def _():
            pump(1, slot + 1, 1)

    place = lax.rem(z, n // S.kv // 2)
    last_place = n // S.kv // 2 - 1
    kv_out = pltpu.make_async_remote_copy(src_ref=kvf, dst_ref=kvg, send_sem=k_s.at[1], recv_sem=k_r.at[1],
                                          device_id={"tp": sib}, device_id_type=MESH)
    parts, lag = KV_PARTS, KV_LAG
    part_rows = S.seq // parts

    def kv_part(i):
        return pl.ds(pl.multiple_of(i * part_rows, part_rows), part_rows)

    def line_copy(way, i):
        src, dst = ((ks, kvl), (vs, kvr))[way]
        to = dev(z + 1) if way == 0 else dev(z - 1)
        return pltpu.make_async_remote_copy(
            src_ref=src.at[kv_part(i)], dst_ref=dst.at[kv_part(i)], send_sem=line_s.at[way, i], recv_sem=line_r.at[way, i],
            device_id={"tp": to}, device_id_type=MESH)

    @pl.when(place == 0)
    def _():
        kvl[...] = jnp.zeros_like(kvl)

    @pl.when(place == last_place)
    def _():
        kvr[...] = jnp.zeros_like(kvr)

    def kv_begin():
        kv_in.wait()
        qs[...] = (qs[...].astype(F32) + kvd[...].astype(F32)).astype(BF)

    def kv_point(p):
        for way in range(2):
            at = place if way == 0 else last_place - place
            i = p - lag * at
            buf, got = ((ks, kvl), (vs, kvr))[way]

            @pl.when(jnp.logical_and(jnp.logical_and(i >= 0, i < parts), at < last_place))
            def _():
                @pl.when(at > 0)
                def _():
                    line_copy(way, i).wait_recv()
                buf[kv_part(i), :] = (qs[kv_part(i), :].astype(F32) + got[kv_part(i), :].astype(F32)).astype(BF)
                line_copy(way, i).start()

    def kv_sum():
        for way in range(2):
            at = place if way == 0 else last_place - place

            @pl.when(at == last_place)
            def _():
                for i in range(parts):
                    line_copy(way, i).wait_recv()
        kvf[...] = (qs[...].astype(F32) + kvl[...].astype(F32) + kvr[...].astype(F32)).astype(BF)
        kv_out.start()

    def kv_last():
        kv_out.wait()

        @pl.loop(0, chips)
        def _(slot):
            for ring in range(2):
                src = pl.ds(pl.multiple_of(block_of(slot, ring) * tok, tok), tok)
                dst = pl.ds(pl.multiple_of(slot * pair + ring * tok, tok), tok)
                dd[dst, S.ak:S.av] = jnp.where(first_core, kvf[src, :], kvg[src, :])
                dd[dst, S.av:S.wa] = jnp.where(first_core, kvg[src, :], kvf[src, :])
        own = pl.multiple_of(lax.rem(me, n // S.kv) * dwk_out.shape[1], 128)
        out = dot_tn(xg[:, pl.ds(own, dwk_out.shape[1])], dd[:, S.ak:S.wa])
        dwk_out[0] = out[:, 0:hd]
        dwv_out[0] = out[:, hd:2 * hd]

    def r_copy(k, sub):
        cut_rows = pl.ds(sub * sub_rows, sub_rows)
        return pltpu.make_async_remote_copy(
            src_ref=rsend.at[lax.rem(k, 2), cut_rows], dst_ref=rrecv.at[k + 1, cut_rows],
            send_sem=r_s.at[k, sub], recv_sem=r_r.at[k + 1, sub], device_id={"tp": nxt}, device_id_type=MESH)

    def d_wait(k):
        dref = drecv.at[k]
        pltpu.make_async_remote_copy(
            src_ref=dref, dst_ref=dref, send_sem=d_s.at[0], recv_sem=d_r.at[k],
            device_id={"tp": sib}, device_id_type=MESH).wait_recv()

    def dx_pump(k, sub):
        @pl.when(k > 0)
        def _():
            rref = rrecv.at[k, pl.ds(sub * sub_rows, sub_rows)]
            pltpu.make_async_remote_copy(
                src_ref=rref, dst_ref=rref, send_sem=r_s.at[0, sub], recv_sem=r_r.at[k, sub],
                device_id={"tp": nxt}, device_id_type=MESH).wait_recv()

        @pl.when(k >= 2)
        def _():
            r_copy(k - 2, sub).wait_send()
        buf = lax.rem(k, 2)
        for g in range(0, sub_rows, 16):
            at = pl.ds(sub * sub_rows + g, 16)
            mine = dxs[buf, pl.ds(pl.multiple_of(c * tok + sub * sub_rows + g, 16), 16), :].astype(F32)
            rsend[buf, at, :] = (mine + drecv[k, at, :].astype(F32) + rrecv[k, at, :].astype(F32)).astype(BF)

        @pl.when(k < chips - 2)
        def _():
            r_copy(k, sub).start()

    whole = fm // 128
    kinds = (
        (0, whole, ((wg_out, None, 0, 128),)), (whole, 2 * whole, ((wu_out, None, 0, 128),)),
        (2 * whole, 2 * whole + 1, ((wq_out, 0, 0, 128),)),
        (2 * whole + 1, 2 * whole + 2, ((wg_out, fm, 0, ft), (wu_out, fm, ft, ft))),
        (2 * whole + 2, 3 * whole + 2, ((wd_out, None, 0, 128),)), (3 * whole + 2, 3 * whole + 3, ((wd_out, fm, 0, ft),)),
        (3 * whole + 3, 3 * whole + 4, ((wo_out, 0, 0, 128),)),
    )
    x_units, units = 2 * whole + 2, 3 * whole + 4
    slots = stage.shape[0]

    def g_do(u, act):
        for lo, hi, pieces in kinds:
            @pl.when(jnp.logical_and(u >= lo, u < hi))
            def _():
                for i, (ref, dst, src, size) in enumerate(pieces):
                    row = pl.multiple_of((u - lo) * 128, 128) if dst is None else dst
                    slot = lax.rem(u, slots)
                    act(pltpu.make_async_copy(stage.at[slot, pl.ds(src, size)], ref.at[pl.ds(row, size)], gsem.at[slot, i]))

    def dw_unit(u):
        @pl.when(jnp.logical_and(u >= slots, u < units))
        def _():
            g_do(u - slots, lambda cp: cp.wait())
        slot = lax.rem(u, slots)
        for lhs, rhs, lo, hi in ((dd, xg, 0, x_units), (hh, yg, x_units, units)):
            @pl.when(jnp.logical_and(u >= lo, u < hi))
            def _():
                at = pl.ds(pl.multiple_of((u - lo) * 128, 128), 128)
                for nb in range(0, d_model, kc):
                    stage[slot, :, nb:nb + kc] = dot_tn(lhs[:, at], rhs[:, nb:nb + kc])
        g_do(u, lambda cp: cp.start())

    kv_begin()
    kv_point(0)

    @pl.loop(0, chips - 1)
    def _(k):
        d_wait(k)
        dx_pump(k, 0)
        kv_point(2 * k + 1)

        @pl.when(k >= 1)
        def _():
            d_copy(k - 1).wait_send()
        dx_part(k + 1)

        dw_unit(3 * k)
        dx_pump(k, 1)
        kv_point(2 * k + 2)

        @pl.when(k == chips - 2)
        def _():
            kv_sum()

        @pl.loop(0, 2)
        def _(i):
            dw_unit(3 * k + 1 + i)

    own_k = chips - 1
    dx_copy = pltpu.make_async_copy(rsend.at[(own_k - 1) % 2], dx_send, lsem.at[0])
    dx_copy.start()
    d_wait(own_k)
    buf = own_k % 2
    for g in range(0, tok, 16):
        mine = dxs[buf, pl.ds(pl.multiple_of(c * tok + g, 16), 16), :].astype(F32)
        dx_own[g:g + 16, :] = mine + drecv[own_k, g:g + 16, :].astype(F32)
    dx_copy.wait()
    kv_last()

    for way in range(2):
        at = place if way == 0 else last_place - place

        @pl.when(at < last_place)
        def _():
            for i in range(parts):
                line_copy(way, i).wait_send()
    for sub in range(SUBS):
        r_copy(chips - 3, sub).wait_send()
    for k in range(chips - 2, chips):
        d_copy(k).wait_send()

    @pl.loop(0, chips)
    def _(slot):
        for st in range(2):
            for sub in range(SUBS):
                @pl.when(slot < chips - 1)
                def _():
                    ring_copy(st, slot, sub, here(st, slot, sub)).wait_send()
                sib_copy(st, slot, sub, here(st, slot, sub)).wait_send()
    for u in range(units - slots, units):
        g_do(jnp.int32(u), lambda cp: cp.wait())


def finish_kernel(wg_hbm, wu_hbm, wd_hbm, wo_hbm, wq_hbm, dwk_hbm, dwv_hbm,
                  wg_out, wu_out, wd_out, wo_out, wq_out, dwk_out, dwv_out,
                  big, wov, wqv, wqt, kvb, isem, osem):
    half = big.shape[1] // 2
    moves = [(wq_hbm, wqv, None, None)]
    for w, (src, dst) in enumerate(((wg_hbm, wg_out), (wu_hbm, wu_out), (wd_hbm, wd_out))):
        for r in (0, half):
            moves.append((src.at[pl.ds(r, half)], big.at[w, pl.ds(r, half)], big.at[w, pl.ds(r, half)], dst.at[pl.ds(r, half)]))
    moves += [(wo_hbm, wov, wov, wo_out), (dwk_hbm, kvb.at[0], kvb.at[0], dwk_out), (dwv_hbm, kvb.at[1], kvb.at[1], dwv_out)]
    moves[0] = (wq_hbm, wqv, wqt, wq_out)
    into = [pltpu.make_async_copy(m[0], m[1], isem.at[i]) for i, m in enumerate(moves)]
    out = [pltpu.make_async_copy(m[2], m[3], osem.at[i]) for i, m in enumerate(moves)]
    for cp in into:
        cp.start()
    for i in range(len(moves)):
        into[i].wait()
        if i == 0:
            wqt[...] = wqv[...].T
        out[i].start()
    for cp in out:
        cp.wait()


def solution(mesh):
    n_dev = mesh.shape["tp"]

    def local_step(x_loc, dy_loc, w_q, w_k, w_v, w_o, w_gate, w_up, w_down):
        tok, d_model = x_loc.shape
        ff, hd, kv = w_gate.shape[1], w_q.shape[2], w_k.shape[1]
        S = Sizes(n_dev, kv, tok, d_model, ff, hd)
        seq, chips, pair = S.seq, S.chips, S.pair
        any_spec = pl.BlockSpec(memory_space=pl.ANY)
        vm = pl.BlockSpec(memory_space=pltpu.VMEM)
        dma = pltpu.SemaphoreType.DMA
        reps = n_dev // kv
        dcut = d_model // reps
        ff_out, hd_out = jax.ShapeDtypeStruct((ff, d_model), F32), jax.ShapeDtypeStruct((hd, d_model), F32)
        kv_out = jax.ShapeDtypeStruct((1, dcut, hd), F32)
        outs = pl.pallas_call(
            functools.partial(fused_kernel, S),
            out_shape=(
                jax.ShapeDtypeStruct((tok, d_model), F32),
                jax.ShapeDtypeStruct((tok, d_model), BF),
                kv_out, kv_out, ff_out, ff_out, hd_out, ff_out, hd_out,
            ),
            in_specs=[any_spec] * 9,
            out_specs=(vm, any_spec, vm, vm) + (any_spec,) * 5,
            scratch_shapes=[
                pltpu.VMEM((seq, d_model), BF), pltpu.VMEM((seq, d_model), BF),
                pltpu.VMEM((S.wa, d_model), BF), pltpu.VMEM((S.wy, d_model), BF),
                pltpu.VMEM((seq, S.wa), BF), pltpu.VMEM((seq, S.wy), BF), pltpu.VMEM((pair, S.fm + 128), F32), pltpu.VMEM((tok, hd), BF),
                pltpu.VMEM((seq, hd), BF), pltpu.VMEM((seq, hd), BF), pltpu.VMEM((seq, hd), BF),
                pltpu.VMEM((tok, seq), BF), pltpu.VMEM((tok, seq), BF),
                pltpu.VMEM((d_model, hd), BF), pltpu.VMEM((2, d_model, kv, hd), BF), pltpu.VMEM((kv * 256, hd), F32),
                pltpu.VMEM((2, pair, d_model), BF), pltpu.VMEM((2, tok, d_model), BF),
                pltpu.VMEM((chips, tok, d_model), BF), pltpu.VMEM((chips, tok, d_model), BF),
                pltpu.VMEM((seq, hd), BF), pltpu.VMEM((seq, hd), BF), pltpu.VMEM((seq, hd), BF),
                pltpu.VMEM((seq, hd), BF), pltpu.VMEM((seq, hd), BF),
                pltpu.VMEM((4, hd, d_model), F32),
                dma((10,)), dma((2, chips, SUBS)), dma((2, chips, SUBS)), dma((2, chips, 2, SUBS)), dma((2,)),
                dma((4, 2)), dma((chips,)), dma((chips,)), dma((chips, SUBS)), dma((chips, SUBS)), dma((2,)), dma((2,)),
                dma((2, KV_PARTS)), dma((2, KV_PARTS)),
            ],
            compiler_params=pltpu.CompilerParams(collective_id=0, has_side_effects=True, vmem_limit_bytes=67043328),
            name="fused",
        )(x_loc, dy_loc, w_q[:, 0, :], w_k, w_v, w_o[0], w_gate.T, w_up.T, w_down)
        dx_own, dx_send, dwk, dwv, wg, wu, wq, wd, wo = outs
        hop = [(i, (i + 2 - 4 * (i % 2)) % n_dev) for i in range(n_dev)]
        dx_last = lax.ppermute(dx_send, "tp", hop)
        wg, wu, wd, wo, wq, dwk, dwv = pl.pallas_call(
            finish_kernel,
            in_specs=[any_spec] * 7,
            out_specs=[any_spec] * 7,
            out_shape=(ff_out, ff_out, ff_out, hd_out, jax.ShapeDtypeStruct((d_model, hd), F32), kv_out, kv_out),
            scratch_shapes=[
                pltpu.VMEM((3, ff, d_model), F32), pltpu.VMEM((hd, d_model), F32), pltpu.VMEM((hd, d_model), F32),
                pltpu.VMEM((d_model, hd), F32), pltpu.VMEM((2, 1, dcut, hd), F32), dma((10,)), dma((10,)),
            ],
            cost_estimate=pl.CostEstimate(flops=10 ** 10, bytes_accessed=38 * 10 ** 6, transcendentals=0),
            compiler_params=pltpu.CompilerParams(vmem_limit_bytes=62 << 20),
            name="finish",
        )(wg, wu, wd, wo, wq, dwk, dwv)
        dx = (dx_own + dx_last.astype(F32)).astype(BF)
        return (dx, wq.reshape(d_model, 1, hd), dwk, dwv, wo[None], wg.T, wu.T, wd)

    token_spec = P(("dp", "tp"), None)
    in_specs = (token_spec, token_spec, P(None, "tp", None), P(None, None, None), P(None, None, None),
                P("tp", None, None), P(None, "tp"), P(None, "tp"), P("tp", None))
    out_specs = (token_spec, P("dp", "tp", None), P(("dp", "tp"), None, None), P(("dp", "tp"), None, None),
                 P(("dp", "tp"), None, None), P("dp", "tp"), P("dp", "tp"), P(("dp", "tp"), None))
    return jax.shard_map(local_step, mesh=mesh, in_specs=in_specs, out_specs=out_specs, check_vma=False)
```

```python
import functools

import jax
import jax.numpy as jnp
from jax import lax
from jax.experimental import pallas as pl
from jax.experimental.pallas import tpu as pltpu
from jax.sharding import PartitionSpec as P

MESH = pl.DeviceIdType.MESH
BF = jnp.bfloat16
F32 = jnp.float32
SUBS = 2
KV_PARTS, KV_LAG = 8, 2


def dot_nt(a, b):
    return lax.dot_general(a, b, (((1,), (1,)), ((), ())), preferred_element_type=F32)


def dot_tn(a, b):
    return lax.dot_general(a, b, (((0,), (0,)), ((), ())), preferred_element_type=F32)


def dot_nn(a, b):
    return jnp.dot(a, b, preferred_element_type=F32)


class Sizes:
    def __init__(self, n_dev, kv_count, tok, d_model, ff, hd):
        self.n, self.kv, self.tok, self.d, self.ff, self.hd = n_dev, kv_count, tok, d_model, ff, hd
        self.chips = n_dev // 2
        self.seq = n_dev * tok
        self.fm = (ff // 128) * 128
        self.ft = ff - self.fm
        assert 0 < 2 * self.ft <= 128 and self.ft % 16 == 0 and hd == 128 and tok == 128
        self.au, self.aq, self.at = self.fm, 2 * self.fm, 2 * self.fm + hd
        self.ak = self.at + 128
        self.av, self.wa = self.ak + hd, self.ak + 2 * hd
        self.yt, self.yo = self.fm, self.fm + 128
        self.wy = self.yo + hd
        self.pair = 2 * tok


def fused_kernel(z_, x_hbm, y_hbm, wq_hbm, wk_hbm, wv_hbm, wo_hbm, wg_hbm, wu_hbm, wd_hbm,
                 dx_own, dx_send, dwk_out, dwv_out, wg_out, wu_out, wq_out, wd_out, wo_out,
                 xg, yg, wall, wy, dd, hh, dhs, dob, qs, ks, vs, pb, ds, wqv, wkv, ktmp,
                 dxs, rsend, drecv, rrecv, kvd, kvl, kvr, kvf, kvg, stage,
                 wsem, ring_s, sib_s, rsem, lsem, osem, gsem, d_s, d_r, r_s, r_r, k_s, k_r, line_s, line_r):
    S = z_
    n, chips, tok, pair, d_model, hd = S.n, S.chips, S.tok, S.pair, S.d, S.hd
    sub_rows = tok // SUBS
    scale = hd ** -0.5
    me = lax.axis_index("tp")
    c = lax.rem(me, 2)
    z = lax.div(me, 2)
    step_dir = 1 - 2 * c
    dev = lambda chip: lax.rem(chip + chips, chips) * 2 + c
    nxt, prv = dev(z + step_dir), dev(z - step_dir)
    sib = me + 1 - 2 * c
    kvi = lax.div(me, n // S.kv)

    barrier = pltpu.get_barrier_semaphore()
    for peer in (sib, nxt, prv):
        pl.semaphore_signal(barrier, inc=1, device_id={"tp": peer}, device_id_type=MESH)

    fm, ft = S.fm, S.ft
    wcopies = [
        pltpu.make_async_copy(wg_hbm.at[pl.ds(0, fm)], wall.at[pl.ds(0, fm)], wsem.at[0]),
        pltpu.make_async_copy(wu_hbm.at[pl.ds(0, fm)], wall.at[pl.ds(S.au, fm)], wsem.at[1]),
        pltpu.make_async_copy(wg_hbm.at[pl.ds(fm, ft)], wall.at[pl.ds(S.at, ft)], wsem.at[2]),
        pltpu.make_async_copy(wu_hbm.at[pl.ds(fm, ft)], wall.at[pl.ds(S.at + ft, ft)], wsem.at[3]),
        pltpu.make_async_copy(wd_hbm.at[pl.ds(0, fm)], wy.at[pl.ds(0, fm)], wsem.at[4]),
        pltpu.make_async_copy(wd_hbm.at[pl.ds(fm, ft)], wy.at[pl.ds(S.yt, ft)], wsem.at[5]),
        pltpu.make_async_copy(wo_hbm, wy.at[pl.ds(S.yo, hd)], wsem.at[6]),
    ]
    qcopy = pltpu.make_async_copy(wq_hbm, wqv, wsem.at[7])
    kcopy = pltpu.make_async_copy(wk_hbm, wkv.at[0], wsem.at[8])
    vcopy = pltpu.make_async_copy(wv_hbm, wkv.at[1], wsem.at[9])
    gathered, owned = (xg, yg), (x_hbm, y_hbm)
    local = [pltpu.make_async_copy(owned[st], gathered[st].at[pl.ds(pl.multiple_of(c * tok, tok), tok)], lsem.at[st])
             for st in range(2)]
    for cp in local + [qcopy, kcopy, vcopy]:
        cp.start()

    def rows(slot, ring, sub):
        return pl.ds(pl.multiple_of(slot * pair + ring * tok + sub * sub_rows, sub_rows), sub_rows)

    def ring_copy(st, slot, sub, src):
        return pltpu.make_async_remote_copy(
            src_ref=src, dst_ref=gathered[st].at[rows(slot + 1, c, sub)],
            send_sem=ring_s.at[st], recv_sem=rsem.at[st, slot + 1, c, sub],
            device_id={"tp": nxt}, device_id_type=MESH)

    def sib_copy(st, slot, sub, src):
        return pltpu.make_async_remote_copy(
            src_ref=src, dst_ref=gathered[st].at[rows(slot, c, sub)],
            send_sem=sib_s.at[st], recv_sem=rsem.at[st, slot, c, sub],
            device_id={"tp": sib}, device_id_type=MESH)

    def here(st, slot, sub):
        return gathered[st].at[rows(slot, c, sub)]

    def wait_block(st, slot, ring, sub):
        ref = gathered[st].at[rows(slot, ring, sub)]
        pltpu.make_async_remote_copy(
            src_ref=ref, dst_ref=ref, send_sem=ring_s.at[st], recv_sem=rsem.at[st, slot, ring, sub],
            device_id={"tp": sib}, device_id_type=MESH).wait_recv()

    def start_ring(st):
        for sub in range(SUBS):
            ring_copy(st, 0, sub, here(st, 0, sub)).start()

    def start_sib(st):
        for sub in range(SUBS):
            sib_copy(st, 0, sub, here(st, 0, sub)).start()

    def pump(st, slot, sub):
        wait_block(st, slot, c, sub)

        @pl.when(slot < chips - 1)
        def _():
            ring_copy(st, slot, sub, here(st, slot, sub)).start()
        sib_copy(st, slot, sub, here(st, slot, sub)).start()

    pl.semaphore_wait(barrier, 3)
    local[0].wait()
    start_ring(0)
    local[1].wait()
    for st in range(2):
        start_sib(st)
    for cp in wcopies:
        cp.start()

    wall[S.at + 2 * ft:S.ak, :] = jnp.zeros((128 - 2 * ft, d_model), BF)
    wy[S.yt + ft:S.yo, :] = jnp.zeros((128 - ft, d_model), BF)
    stage[1] = jnp.zeros(stage.shape[1:], F32)
    rrecv[0] = jnp.zeros(rrecv.shape[1:], BF)
    qcopy.wait()
    kcopy.wait()
    vcopy.wait()
    span = 256

    @pl.loop(0, d_model // span)
    def _(i):
        r0 = pl.multiple_of(i * span, span)
        wall[S.aq:S.aq + hd, pl.ds(r0, span)] = wqv[pl.ds(r0, span), :].T
        for w in range(2):
            ktmp[...] = wkv[w, pl.ds(r0, span)].reshape(S.kv * span, hd).astype(F32)
            one = ktmp[pl.ds(kvi, span, stride=S.kv), :]
            off = S.ak + w * hd
            wall[off:off + hd, pl.ds(r0, span)] = one.T.astype(BF)
    pump(0, 1, 0)
    for cp in wcopies:
        cp.wait()

    def block_of(slot, ring):
        chip = lax.rem(z + chips + jnp.where(ring == 0, -slot, slot), chips)
        return chip * 2 + ring

    def slot_rows(slot):
        return pl.ds(pl.multiple_of(slot * pair, pair), pair)

    cut = 1024

    def fwd_first(slot):
        out = dot_nt(xg[slot_rows(slot), :], wall[0:cut, :])
        dd[slot_rows(slot), 0:cut] = out.astype(BF)

    def fwd_second(slot):
        out = dot_nt(xg[slot_rows(slot), :], wall[cut:S.wa, :]).astype(BF)
        dd[slot_rows(slot), cut:S.wa] = out
        for ring in range(2):
            tgt = pl.ds(pl.multiple_of(block_of(slot, ring) * tok, tok), tok)
            part = out[ring * tok:(ring + 1) * tok]
            qs[tgt, :] = part[:, S.aq - cut:S.at - cut]
            ks[tgt, :] = part[:, S.ak - cut:S.av - cut]
            vs[tgt, :] = part[:, S.av - cut:S.wa - cut]

    lane = lax.broadcasted_iota(jnp.int32, (32, 128), 1)

    def mlp_mid(slot):
        @pl.loop(0, pair // 32)
        def _(i):
            r = pl.ds(pl.multiple_of(slot * pair + i * 32, 32), 32)
            rl = pl.ds(pl.multiple_of(i * 32, 32), 32)

            def grads(a, u, dh):
                sg = jax.nn.sigmoid(a)
                act = a * sg
                return act * u, dh * u * sg * (1.0 + a * (1.0 - sg)), dh * act

            for j in range(0, fm, 128):
                h, da, du = grads(dd[r, j:j + 128].astype(F32), dd[r, S.au + j:S.au + j + 128].astype(F32), dhs[rl, j:j + 128])
                hh[r, j:j + 128] = h.astype(BF)
                dd[r, j:j + 128] = da.astype(BF)
                dd[r, S.au + j:S.au + j + 128] = du.astype(BF)
            both = dd[r, S.at:S.ak].astype(F32)
            h, da, du = grads(both, pltpu.roll(both, 128 - ft, 1), dhs[rl, fm:fm + 128])
            hh[r, S.yt:S.yo] = h.astype(BF)
            rest = jnp.where(lane < ft, da, jnp.where(lane < 2 * ft, pltpu.roll(du, ft, 1), 0.0))
            dd[r, S.at:S.ak] = rest.astype(BF)

    def y_out(slot, ring):
        part = pl.ds(pl.multiple_of(slot * pair + ring * tok, tok), tok)
        dob[...] = dot_nt(yg[part, :], wy[S.yo:S.wy, :]).astype(BF)

    def y_first(slot):
        dhs[...] = dot_nt(yg[slot_rows(slot), :], wy[0:S.yo, :])

    for sub in range(SUBS):
        wait_block(1, 0, 1 - c, sub)
    y_first(0)

    @pl.loop(0, chips)
    def _(slot):
        for sub in range(SUBS):
            wait_block(0, slot, 1 - c, sub)
        fwd_first(slot)

        @pl.when(slot < chips - 1)
        def _():
            pump(0, slot + 1, 1)

        @pl.when(slot == chips - 3)
        def _():
            start_ring(1)

        @pl.when(slot == chips - 1)
        def _():
            pump(1, 1, 0)
        fwd_second(slot)

        @pl.when(slot == 0)
        def _():
            mlp_mid(0)

        @pl.when(slot < chips - 2)
        def _():
            pump(0, slot + 2, 0)

    kc = 256
    sc, dka, dva = stage.at[0, pl.ds(0, tok)], stage.at[1, pl.ds(0, tok)], stage.at[1, pl.ds(tok, tok)]

    def attend(slot, ring, blk, chunks):
        qrow = pl.ds(pl.multiple_of(blk * tok, tok), tok)
        q = qs[qrow, :]
        dout = dob[...]
        srow = pl.ds(pl.multiple_of(slot * pair + ring * tok, tok), tok)
        run = None
        for ch in range(chunks):
            s = dot_nt(q, ks[ch * kc:(ch + 1) * kc, :]) * scale
            if ch >= chunks - 2:
                col = lax.broadcasted_iota(jnp.int32, (tok, kc), 1) + ch * kc
                row = lax.broadcasted_iota(jnp.int32, (tok, kc), 0) + blk * tok
                s = jnp.where(col <= row, s, -jnp.inf)
            sc[:, ch * kc:(ch + 1) * kc] = s
            top = jnp.maximum(s[:, 0:128], s[:, 128:256])
            run = top if run is None else jnp.maximum(run, top)
        m = jnp.max(run, axis=1, keepdims=True)
        tot = jnp.zeros((tok, 128), F32)
        for ch in range(chunks):
            p = jnp.exp(sc[:, ch * kc:(ch + 1) * kc] - m)
            sc[:, ch * kc:(ch + 1) * kc] = p
            tot = tot + p[:, 0:128] + p[:, 128:256]
        inv = 1.0 / jnp.sum(tot, axis=1, keepdims=True)
        for ch in range(chunks):
            p = sc[:, ch * kc:(ch + 1) * kc] * inv
            sc[:, ch * kc:(ch + 1) * kc] = p
            pb[:, ch * kc:(ch + 1) * kc] = p.astype(BF)
        length = chunks * kc
        o = dot_nn(pb[:, 0:length], vs[0:length, :]).astype(BF)
        hh[srow, S.yo:S.wy] = o
        delta = jnp.sum(dout.astype(F32) * o.astype(F32), axis=1, keepdims=True)
        for ch in range(chunks):
            dp = dot_nt(dout, vs[ch * kc:(ch + 1) * kc, :])
            ds[:, ch * kc:(ch + 1) * kc] = (sc[:, ch * kc:(ch + 1) * kc] * (dp - delta)).astype(BF)
        dq = dot_nn(ds[:, 0:length], ks[0:length, :]) * scale
        dd[srow, S.aq:S.at] = dq.astype(BF)
        for ch in range(chunks):
            for acc, lhs, rhs in ((dka, ds, q), (dva, pb, dout)):
                acc[:, ch * kc:(ch + 1) * kc] += dot_tn(rhs, lhs[:, ch * kc:(ch + 1) * kc])

    def attend_ring(slot, ring):
        blk = block_of(slot, ring)
        group = lax.div(blk, 4)
        for v in range(n // 4):
            @pl.when(group == v)
            def _():
                attend(slot, ring, blk, 2 * (v + 1))

    first_core = c == 0
    kv_in = pltpu.make_async_remote_copy(src_ref=ks, dst_ref=kvd, send_sem=k_s.at[0], recv_sem=k_r.at[0],
                                         device_id={"tp": sib}, device_id_type=MESH)

    def kv_own():
        for slot in range(chips):
            for ring in range(2):
                at = pl.multiple_of(block_of(slot, ring) * tok, tok)
                dst = slice(slot * pair + ring * tok, slot * pair + (ring + 1) * tok)
                dk = (dka[:, pl.ds(at, tok)] * scale).astype(BF).T
                dv = dva[:, pl.ds(at, tok)].astype(BF).T
                dd[dst, S.ak:S.av] = dk
                dd[dst, S.av:S.wa] = dv
                qs[pl.ds(at, tok), :] = jnp.where(first_core, dk, dv)
                ks[pl.ds(at, tok), :] = jnp.where(first_core, dv, dk)
        kv_in.start()

    def d_copy(k):
        return pltpu.make_async_remote_copy(
            src_ref=dxs.at[lax.rem(k, 2), pl.ds(pl.multiple_of((1 - c) * tok, tok), tok)], dst_ref=drecv.at[k],
            send_sem=d_s.at[k], recv_sem=d_r.at[k], device_id={"tp": sib}, device_id_type=MESH)

    def dx_main(k, part):
        at = pl.ds(pl.multiple_of(part * (d_model // 2), 1024), d_model // 2)
        out = dot_nn(dd[slot_rows(k + 1), 0:S.ak], wall[0:S.ak, at])
        dxs[k, :, at] = out.astype(BF)

    def dx_kv(k):
        lhs = dd[slice((k + 1) * pair, (k + 2) * pair), S.ak:S.wa]
        for nb in range(0, d_model, 512):
            out = dot_nn(lhs, wall[S.ak:S.wa, nb:nb + 512])
            dxs[k, :, nb:nb + 512] = (dxs[k, :, nb:nb + 512].astype(F32) + out).astype(BF)
        d_copy(jnp.int32(k)).start()

    def dx_part(k):
        buf = lax.rem(k, 2)
        lhs = dd[slot_rows(lax.rem(k + 1, chips)), :]
        for nb in range(0, d_model, 512):
            dxs[buf, :, nb:nb + 512] = dot_nn(lhs, wall[:, nb:nb + 512]).astype(BF)
        d_copy(k).start()

    @pl.loop(0, chips)
    def _(slot):
        y_out(slot, c)
        attend_ring(slot, c)

        @pl.when(jnp.logical_and(slot >= 3, slot < 7))
        def _():
            dx_main(lax.div(slot - 3, 2), lax.rem(slot - 3, 2))

        @pl.when(jnp.logical_and(slot > 0, slot < chips - 1))
        def _():
            pump(1, slot + 1, 0)

        @pl.when(slot > 0)
        def _():
            for sub in range(SUBS):
                wait_block(1, slot, 1 - c, sub)
        y_out(slot, 1 - c)
        attend_ring(slot, 1 - c)

        @pl.when(slot == chips - 1)
        def _():
            kv_own()
            dx_kv(0)

        @pl.when(slot > 0)
        def _():
            y_first(slot)
            mlp_mid(slot)

        @pl.when(slot < chips - 1)
        def _():
            pump(1, slot + 1, 1)

    place = lax.rem(z, n // S.kv // 2)
    last_place = n // S.kv // 2 - 1
    kv_out = pltpu.make_async_remote_copy(src_ref=kvf, dst_ref=kvg, send_sem=k_s.at[1], recv_sem=k_r.at[1],
                                          device_id={"tp": sib}, device_id_type=MESH)
    parts, lag = KV_PARTS, KV_LAG
    part_rows = S.seq // parts

    def kv_part(i):
        return pl.ds(pl.multiple_of(i * part_rows, part_rows), part_rows)

    def line_copy(way, i):
        src, dst = ((ks, kvl), (vs, kvr))[way]
        to = dev(z + 1) if way == 0 else dev(z - 1)
        return pltpu.make_async_remote_copy(
            src_ref=src.at[kv_part(i)], dst_ref=dst.at[kv_part(i)], send_sem=line_s.at[way, i], recv_sem=line_r.at[way, i],
            device_id={"tp": to}, device_id_type=MESH)

    @pl.when(place == 0)
    def _():
        kvl[...] = jnp.zeros_like(kvl)

    @pl.when(place == last_place)
    def _():
        kvr[...] = jnp.zeros_like(kvr)

    def kv_begin():
        kv_in.wait()
        qs[...] = (qs[...].astype(F32) + kvd[...].astype(F32)).astype(BF)

    def kv_point(p):
        for way in range(2):
            at = place if way == 0 else last_place - place
            i = p + 1 - lag * at
            buf, got = ((ks, kvl), (vs, kvr))[way]

            @pl.when(jnp.logical_and(jnp.logical_and(i >= 0, i < parts), at < last_place))
            def _():
                @pl.when(at > 0)
                def _():
                    line_copy(way, i).wait_recv()
                buf[kv_part(i), :] = (qs[kv_part(i), :].astype(F32) + got[kv_part(i), :].astype(F32)).astype(BF)
                line_copy(way, i).start()

    def kv_sum():
        for way in range(2):
            at = place if way == 0 else last_place - place

            @pl.when(at == last_place)
            def _():
                for i in range(parts):
                    line_copy(way, i).wait_recv()
        kvf[...] = (qs[...].astype(F32) + kvl[...].astype(F32) + kvr[...].astype(F32)).astype(BF)
        kv_out.start()

    def kv_last():
        kv_out.wait()

        @pl.loop(0, chips)
        def _(slot):
            for ring in range(2):
                src = pl.ds(pl.multiple_of(block_of(slot, ring) * tok, tok), tok)
                dst = pl.ds(pl.multiple_of(slot * pair + ring * tok, tok), tok)
                dd[dst, S.ak:S.av] = jnp.where(first_core, kvf[src, :], kvg[src, :])
                dd[dst, S.av:S.wa] = jnp.where(first_core, kvg[src, :], kvf[src, :])
        own = pl.multiple_of(lax.rem(me, n // S.kv) * dwk_out.shape[1], 128)
        out = dot_tn(xg[:, pl.ds(own, dwk_out.shape[1])], dd[:, S.ak:S.wa])
        dhs[:, 0:2 * hd] = out

    def r_copy(k, sub):
        cut_rows = pl.ds(sub * sub_rows, sub_rows)
        return pltpu.make_async_remote_copy(
            src_ref=rsend.at[lax.rem(k, 2), cut_rows], dst_ref=rrecv.at[k + 1, cut_rows],
            send_sem=r_s.at[k, sub], recv_sem=r_r.at[k + 1, sub], device_id={"tp": nxt}, device_id_type=MESH)

    def d_wait(k):
        dref = drecv.at[k]
        pltpu.make_async_remote_copy(
            src_ref=dref, dst_ref=dref, send_sem=d_s.at[0], recv_sem=d_r.at[k],
            device_id={"tp": sib}, device_id_type=MESH).wait_recv()

    def dx_pump(k, sub):
        @pl.when(k > 0)
        def _():
            rref = rrecv.at[k, pl.ds(sub * sub_rows, sub_rows)]
            pltpu.make_async_remote_copy(
                src_ref=rref, dst_ref=rref, send_sem=r_s.at[0, sub], recv_sem=r_r.at[k, sub],
                device_id={"tp": nxt}, device_id_type=MESH).wait_recv()

        @pl.when(k >= 2)
        def _():
            r_copy(k - 2, sub).wait_send()
        buf = lax.rem(k, 2)
        for g in range(0, sub_rows, 16):
            at = pl.ds(sub * sub_rows + g, 16)
            mine = dxs[buf, pl.ds(pl.multiple_of(c * tok + sub * sub_rows + g, 16), 16), :].astype(F32)
            rsend[buf, at, :] = (mine + drecv[k, at, :].astype(F32) + rrecv[k, at, :].astype(F32)).astype(BF)

        @pl.when(k < chips - 2)
        def _():
            r_copy(k, sub).start()

    rows_of = (
        ((wo_out, 0, 0, hd),),
        ((wg_out, 0, 0, kc),), ((wg_out, kc, 0, kc),), ((wg_out, 2 * kc, 0, fm - 2 * kc), (wu_out, 0, fm - 2 * kc, 3 * kc - fm)),
        ((wu_out, 3 * kc - fm, 0, kc),), ((wu_out, 4 * kc - fm, 0, kc),),
        ((wq_out, 0, 0, hd), (wg_out, fm, hd, ft), (wu_out, fm, hd + ft, ft)),
        ((wd_out, 0, 0, kc),), ((wd_out, kc, 0, kc),), ((wd_out, 2 * kc, 0, fm - 2 * kc), (wd_out, fm, fm - 2 * kc, ft)),
    )
    units, x_end = len(rows_of), 7

    def g_copies(u):
        return [pltpu.make_async_copy(stage.at[u % 2, pl.ds(src, size)], ref.at[pl.ds(dst, size)], gsem.at[u % 2, i])
                for i, (ref, dst, src, size) in enumerate(rows_of[u])]

    def dw_unit(u):
        for w in range(2, units):
            @pl.when(u == w)
            def _():
                for cp in g_copies(w - 2):
                    cp.wait()
        buf = lax.rem(u, 2)

        @pl.when(u == 0)
        def _():
            for nb in range(0, d_model, kc):
                stage[0, 0:hd, nb:nb + kc] = dot_tn(hh[:, S.yo:S.wy], yg[:, nb:nb + kc])
        for lhs, rhs, lo, hi in ((dd, xg, 1, x_end), (hh, yg, x_end, units)):
            @pl.when(jnp.logical_and(u >= lo, u < hi))
            def _():
                at = pl.ds(pl.multiple_of((u - lo) * kc, kc), kc)
                for nb in range(0, d_model, kc):
                    stage[buf, :, nb:nb + kc] = dot_tn(lhs[:, at], rhs[:, nb:nb + kc])
        for w in range(units):
            @pl.when(u == w)
            def _():
                for cp in g_copies(w):
                    cp.start()

    own_k = chips - 1

    def own_tokens():
        d_wait(own_k)
        for g in range(0, tok, 16):
            mine = dxs[own_k % 2, pl.ds(pl.multiple_of(c * tok + g, 16), 16), :].astype(F32)
            pb[g:g + 16, :] = (mine + drecv[own_k, g:g + 16, :].astype(F32)).astype(BF)

    last = [pltpu.make_async_copy(pb, dx_own, osem.at[0]),
            pltpu.make_async_copy(dhs.at[:, pl.ds(0, hd)], dwk_out.at[0], osem.at[1]),
            pltpu.make_async_copy(dhs.at[:, pl.ds(hd, hd)], dwv_out.at[0], osem.at[2]),
            pltpu.make_async_copy(rsend.at[(own_k - 1) % 2], dx_send, osem.at[3])]

    kv_begin()
    kv_point(-1)
    kv_point(0)

    @pl.loop(0, chips - 1)
    def _(k):
        d_wait(k)
        dx_pump(k, 0)
        kv_point(2 * k + 1)

        @pl.when(k == 0)
        def _():
            dx_kv(1)

        @pl.when(k >= 1)
        def _():
            d_copy(k - 1).wait_send()
            dx_part(k + 1)

        @pl.when(jnp.logical_and(k >= 2, k < chips - 3))
        def _():
            dw_unit(2 * k - 1)

        @pl.when(k == chips - 2)
        def _():
            kv_last()
            last[1].start()
            last[2].start()
            own_tokens()
            last[0].start()
        dx_pump(k, 1)
        kv_point(2 * k + 2)

        @pl.loop(0, jnp.where(k == 0, 2, jnp.where(k < chips - 2, 1, 0)))
        def _(i):
            dw_unit(jnp.where(k == 0, i, jnp.minimum(2 * k, units - 1)))

        @pl.when(k == chips - 3)
        def _():
            kv_sum()

    last[3].start()
    for cp in last:
        cp.wait()

    for way in range(2):
        at = place if way == 0 else last_place - place

        @pl.when(at < last_place)
        def _():
            for i in range(parts):
                line_copy(way, i).wait_send()
    for sub in range(SUBS):
        r_copy(chips - 3, sub).wait_send()
    for k in range(chips - 2, chips):
        d_copy(k).wait_send()

    for st in range(2):
        for sem, count in ((ring_s, chips - 1), (sib_s, chips)):
            span_all = gathered[st].at[pl.ds(0, count * tok)]
            pltpu.make_async_remote_copy(
                src_ref=span_all, dst_ref=span_all, send_sem=sem.at[st], recv_sem=rsem.at[st, 0, 0, 0],
                device_id={"tp": sib}, device_id_type=MESH).wait_send()
    for u in range(units - 2, units):
        for cp in g_copies(u):
            cp.wait()


def finish_kernel(wg_hbm, wu_hbm, wd_hbm, wo_hbm, wq_hbm, dwk_hbm, dwv_hbm,
                  wg_out, wu_out, wd_out, wo_out, wq_out, dwk_out, dwv_out,
                  big, wov, wqv, wqt, kvb, isem, osem):
    half = big.shape[1] // 2
    moves = [(wq_hbm, wqv, None, None)]
    for w, (src, dst) in enumerate(((wg_hbm, wg_out), (wu_hbm, wu_out), (wd_hbm, wd_out))):
        for r in (0, half):
            moves.append((src.at[pl.ds(r, half)], big.at[w, pl.ds(r, half)], big.at[w, pl.ds(r, half)], dst.at[pl.ds(r, half)]))
    moves += [(wo_hbm, wov, wov, wo_out), (dwk_hbm, kvb.at[0], kvb.at[0], dwk_out), (dwv_hbm, kvb.at[1], kvb.at[1], dwv_out)]
    moves[0] = (wq_hbm, wqv, wqt, wq_out)
    into = [pltpu.make_async_copy(m[0], m[1], isem.at[i]) for i, m in enumerate(moves)]
    out = [pltpu.make_async_copy(m[2], m[3], osem.at[i]) for i, m in enumerate(moves)]
    for cp in into:
        cp.start()
    for i in range(len(moves)):
        into[i].wait()
        if i == 0:
            wqt[...] = wqv[...].T
        out[i].start()
    for cp in out:
        cp.wait()


def solution(mesh):
    n_dev = mesh.shape["tp"]

    def local_step(x_loc, dy_loc, w_q, w_k, w_v, w_o, w_gate, w_up, w_down):
        tok, d_model = x_loc.shape
        ff, hd, kv = w_gate.shape[1], w_q.shape[2], w_k.shape[1]
        S = Sizes(n_dev, kv, tok, d_model, ff, hd)
        seq, chips, pair = S.seq, S.chips, S.pair
        any_spec = pl.BlockSpec(memory_space=pl.ANY)
        dma = pltpu.SemaphoreType.DMA
        reps = n_dev // kv
        dcut = d_model // reps
        ff_out, hd_out = jax.ShapeDtypeStruct((ff, d_model), F32), jax.ShapeDtypeStruct((hd, d_model), F32)
        kv_out = jax.ShapeDtypeStruct((1, dcut, hd), F32)
        outs = pl.pallas_call(
            functools.partial(fused_kernel, S),
            out_shape=(
                jax.ShapeDtypeStruct((tok, d_model), BF),
                jax.ShapeDtypeStruct((tok, d_model), BF),
                kv_out, kv_out, ff_out, ff_out, hd_out, ff_out, hd_out,
            ),
            in_specs=[any_spec] * 9,
            out_specs=[any_spec] * 9,
            scratch_shapes=[
                pltpu.VMEM((seq, d_model), BF), pltpu.VMEM((seq, d_model), BF),
                pltpu.VMEM((S.wa, d_model), BF), pltpu.VMEM((S.wy, d_model), BF),
                pltpu.VMEM((seq, S.wa), BF), pltpu.VMEM((seq, S.wy), BF), pltpu.VMEM((pair, S.fm + 128), F32), pltpu.VMEM((tok, hd), BF),
                pltpu.VMEM((seq, hd), BF), pltpu.VMEM((seq, hd), BF), pltpu.VMEM((seq, hd), BF),
                pltpu.VMEM((tok, seq), BF), pltpu.VMEM((tok, seq), BF),
                pltpu.VMEM((d_model, hd), BF), pltpu.VMEM((2, d_model, kv, hd), BF), pltpu.VMEM((kv * 256, hd), F32),
                pltpu.VMEM((2, pair, d_model), BF), pltpu.VMEM((2, tok, d_model), BF),
                pltpu.VMEM((chips, tok, d_model), BF), pltpu.VMEM((chips, tok, d_model), BF),
                pltpu.VMEM((seq, hd), BF), pltpu.VMEM((seq, hd), BF), pltpu.VMEM((seq, hd), BF),
                pltpu.VMEM((seq, hd), BF), pltpu.VMEM((seq, hd), BF),
                pltpu.VMEM((2, 2 * hd, d_model), F32),
                dma((10,)), dma((2,)), dma((2,)), dma((2, chips, 2, SUBS)), dma((2,)), dma((4,)),
                dma((2, 3)), dma((chips,)), dma((chips,)), dma((chips, SUBS)), dma((chips, SUBS)), dma((2,)), dma((2,)),
                dma((2, KV_PARTS)), dma((2, KV_PARTS)),
            ],
            compiler_params=pltpu.CompilerParams(collective_id=0, has_side_effects=True, vmem_limit_bytes=67043328),
            name="fused",
        )(x_loc, dy_loc, w_q[:, 0, :], w_k, w_v, w_o[0], w_gate.T, w_up.T, w_down)
        dx_own, dx_send, dwk, dwv, wg, wu, wq, wd, wo = outs
        hop = [(i, (i + 2 - 4 * (i % 2)) % n_dev) for i in range(n_dev)]
        dx_last = lax.ppermute(dx_send, "tp", hop)
        wg, wu, wd, wo, wq, dwk, dwv = pl.pallas_call(
            finish_kernel,
            in_specs=[any_spec] * 7,
            out_specs=[any_spec] * 7,
            out_shape=(ff_out, ff_out, ff_out, hd_out, jax.ShapeDtypeStruct((d_model, hd), F32), kv_out, kv_out),
            scratch_shapes=[
                pltpu.VMEM((3, ff, d_model), F32), pltpu.VMEM((hd, d_model), F32), pltpu.VMEM((hd, d_model), F32),
                pltpu.VMEM((d_model, hd), F32), pltpu.VMEM((2, 1, dcut, hd), F32), dma((10,)), dma((10,)),
            ],
            cost_estimate=pl.CostEstimate(flops=10 ** 10, bytes_accessed=38 * 10 ** 6, transcendentals=0),
            compiler_params=pltpu.CompilerParams(vmem_limit_bytes=62 << 20),
            name="finish",
        )(wg, wu, wd, wo, wq, dwk, dwv)
        dx = (dx_own.astype(F32) + dx_last.astype(F32)).astype(BF)
        return (dx, wq.reshape(d_model, 1, hd), dwk, dwv, wo[None], wg.T, wu.T, wd)

    token_spec = P(("dp", "tp"), None)
    in_specs = (token_spec, token_spec, P(None, "tp", None), P(None, None, None), P(None, None, None),
                P("tp", None, None), P(None, "tp"), P(None, "tp"), P("tp", None))
    out_specs = (token_spec, P("dp", "tp", None), P(("dp", "tp"), None, None), P(("dp", "tp"), None, None),
                 P(("dp", "tp"), None, None), P("dp", "tp"), P("dp", "tp"), P(("dp", "tp"), None))
    return jax.shard_map(local_step, mesh=mesh, in_specs=in_specs, out_specs=out_specs, check_vma=False)
```

```python
import functools

import jax
import jax.numpy as jnp
from jax import lax
from jax.experimental import pallas as pl
from jax.experimental.pallas import tpu as pltpu
from jax.sharding import PartitionSpec as P

MESH = pl.DeviceIdType.MESH
BF = jnp.bfloat16
F32 = jnp.float32
SUBS = 2
KV_PARTS, KV_LAG = 8, 2


def dot_nt(a, b):
    return lax.dot_general(a, b, (((1,), (1,)), ((), ())), preferred_element_type=F32)


def dot_tn(a, b):
    return lax.dot_general(a, b, (((0,), (0,)), ((), ())), preferred_element_type=F32)


def dot_nn(a, b):
    return jnp.dot(a, b, preferred_element_type=F32)


class Sizes:
    def __init__(self, n_dev, kv_count, tok, d_model, ff, hd):
        self.n, self.kv, self.tok, self.d, self.ff, self.hd = n_dev, kv_count, tok, d_model, ff, hd
        self.chips = n_dev // 2
        self.seq = n_dev * tok
        self.fm = (ff // 128) * 128
        self.ft = ff - self.fm
        assert 0 < 2 * self.ft <= 128 and self.ft % 16 == 0 and hd == 128 and tok == 128
        self.au, self.aq, self.at = self.fm, 2 * self.fm, 2 * self.fm + hd
        self.ak = self.at + 128
        self.av, self.wa = self.ak + hd, self.ak + 2 * hd
        self.yt, self.yo = self.fm, self.fm + 128
        self.wy = self.yo + hd
        self.pair = 2 * tok


def fused_kernel(z_, x_hbm, y_hbm, wq_hbm, wk_hbm, wv_hbm, wo_hbm, wg_hbm, wu_hbm, wd_hbm,
                 dx_own, dx_send, dwk_out, dwv_out, wg_out, wu_out, wq_out, wd_out, wo_out,
                 xg, yg, wall, wy, dd, hh, dhs, dob, qs, ks, vs, pb, ds, wqv, wkv, ktmp,
                 dxs, rsend, drecv, rrecv, kvd, kvl, kvr, kvf, kvg, stage,
                 wsem, ring_s, sib_s, rsem, lsem, osem, gsem, d_s, d_r, r_s, r_r, k_s, k_r, line_s, line_r):
    S = z_
    n, chips, tok, pair, d_model, hd = S.n, S.chips, S.tok, S.pair, S.d, S.hd
    sub_rows = tok // SUBS
    scale = hd ** -0.5
    me = lax.axis_index("tp")
    c = lax.rem(me, 2)
    z = lax.div(me, 2)
    step_dir = 1 - 2 * c
    dev = lambda chip: lax.rem(chip + chips, chips) * 2 + c
    nxt, prv = dev(z + step_dir), dev(z - step_dir)
    sib = me + 1 - 2 * c
    kvi = lax.div(me, n // S.kv)

    barrier = pltpu.get_barrier_semaphore()
    for peer in (sib, nxt, prv):
        pl.semaphore_signal(barrier, inc=1, device_id={"tp": peer}, device_id_type=MESH)

    fm, ft = S.fm, S.ft
    wcopies = [
        pltpu.make_async_copy(wg_hbm.at[pl.ds(0, fm)], wall.at[pl.ds(0, fm)], wsem.at[0]),
        pltpu.make_async_copy(wu_hbm.at[pl.ds(0, fm)], wall.at[pl.ds(S.au, fm)], wsem.at[1]),
        pltpu.make_async_copy(wg_hbm.at[pl.ds(fm, ft)], wall.at[pl.ds(S.at, ft)], wsem.at[2]),
        pltpu.make_async_copy(wu_hbm.at[pl.ds(fm, ft)], wall.at[pl.ds(S.at + ft, ft)], wsem.at[3]),
        pltpu.make_async_copy(wd_hbm.at[pl.ds(0, fm)], wy.at[pl.ds(0, fm)], wsem.at[4]),
        pltpu.make_async_copy(wd_hbm.at[pl.ds(fm, ft)], wy.at[pl.ds(S.yt, ft)], wsem.at[5]),
        pltpu.make_async_copy(wo_hbm, wy.at[pl.ds(S.yo, hd)], wsem.at[6]),
    ]
    qcopy = pltpu.make_async_copy(wq_hbm, wqv, wsem.at[7])
    kcopy = pltpu.make_async_copy(wk_hbm, wkv.at[0], wsem.at[8])
    vcopy = pltpu.make_async_copy(wv_hbm, wkv.at[1], wsem.at[9])
    gathered, owned = (xg, yg), (x_hbm, y_hbm)
    local = [pltpu.make_async_copy(owned[st], gathered[st].at[pl.ds(pl.multiple_of(c * tok, tok), tok)], lsem.at[st])
             for st in range(2)]
    for cp in local + [qcopy, kcopy, vcopy]:
        cp.start()

    def rows(slot, ring, sub):
        return pl.ds(pl.multiple_of(slot * pair + ring * tok + sub * sub_rows, sub_rows), sub_rows)

    def ring_copy(st, slot, sub, src):
        return pltpu.make_async_remote_copy(
            src_ref=src, dst_ref=gathered[st].at[rows(slot + 1, c, sub)],
            send_sem=ring_s.at[st], recv_sem=rsem.at[st, slot + 1, c, sub],
            device_id={"tp": nxt}, device_id_type=MESH)

    def sib_copy(st, slot, sub, src):
        return pltpu.make_async_remote_copy(
            src_ref=src, dst_ref=gathered[st].at[rows(slot, c, sub)],
            send_sem=sib_s.at[st], recv_sem=rsem.at[st, slot, c, sub],
            device_id={"tp": sib}, device_id_type=MESH)

    def here(st, slot, sub):
        return gathered[st].at[rows(slot, c, sub)]

    def wait_block(st, slot, ring, sub):
        ref = gathered[st].at[rows(slot, ring, sub)]
        pltpu.make_async_remote_copy(
            src_ref=ref, dst_ref=ref, send_sem=ring_s.at[st], recv_sem=rsem.at[st, slot, ring, sub],
            device_id={"tp": sib}, device_id_type=MESH).wait_recv()

    def start_ring(st):
        for sub in range(SUBS):
            ring_copy(st, 0, sub, here(st, 0, sub)).start()

    def start_sib(st):
        for sub in range(SUBS):
            sib_copy(st, 0, sub, here(st, 0, sub)).start()

    def pump(st, slot, sub):
        wait_block(st, slot, c, sub)

        @pl.when(slot < chips - 1)
        def _():
            ring_copy(st, slot, sub, here(st, slot, sub)).start()
        sib_copy(st, slot, sub, here(st, slot, sub)).start()

    pl.semaphore_wait(barrier, 3)
    local[0].wait()
    start_ring(0)
    local[1].wait()
    for st in range(2):
        start_sib(st)
    for cp in wcopies:
        cp.start()

    wall[S.at + 2 * ft:S.ak, :] = jnp.zeros((128 - 2 * ft, d_model), BF)
    wy[S.yt + ft:S.yo, :] = jnp.zeros((128 - ft, d_model), BF)
    stage[1] = jnp.zeros(stage.shape[1:], F32)
    rrecv[0] = jnp.zeros(rrecv.shape[1:], BF)
    qcopy.wait()
    kcopy.wait()
    vcopy.wait()
    span = 256

    @pl.loop(0, d_model // span)
    def _(i):
        r0 = pl.multiple_of(i * span, span)
        wall[S.aq:S.aq + hd, pl.ds(r0, span)] = wqv[pl.ds(r0, span), :].T
        for w in range(2):
            ktmp[...] = wkv[w, pl.ds(r0, span)].reshape(S.kv * span, hd).astype(F32)
            one = ktmp[pl.ds(kvi, span, stride=S.kv), :]
            off = S.ak + w * hd
            wall[off:off + hd, pl.ds(r0, span)] = one.T.astype(BF)
    pump(0, 1, 0)
    for cp in wcopies:
        cp.wait()

    def block_of(slot, ring):
        chip = lax.rem(z + chips + jnp.where(ring == 0, -slot, slot), chips)
        return chip * 2 + ring

    def slot_rows(slot):
        return pl.ds(pl.multiple_of(slot * pair, pair), pair)

    cut = 1024

    def fwd_first(slot):
        out = dot_nt(xg[slot_rows(slot), :], wall[0:cut, :])
        dd[slot_rows(slot), 0:cut] = out.astype(BF)

    def fwd_second(slot):
        out = dot_nt(xg[slot_rows(slot), :], wall[cut:S.wa, :]).astype(BF)
        dd[slot_rows(slot), cut:S.wa] = out
        for ring in range(2):
            tgt = pl.ds(pl.multiple_of(block_of(slot, ring) * tok, tok), tok)
            part = out[ring * tok:(ring + 1) * tok]
            qs[tgt, :] = part[:, S.aq - cut:S.at - cut]
            ks[tgt, :] = part[:, S.ak - cut:S.av - cut]
            vs[tgt, :] = part[:, S.av - cut:S.wa - cut]

    lane = lax.broadcasted_iota(jnp.int32, (32, 128), 1)

    def mlp_mid(slot):
        @pl.loop(0, pair // 32)
        def _(i):
            r = pl.ds(pl.multiple_of(slot * pair + i * 32, 32), 32)
            rl = pl.ds(pl.multiple_of(i * 32, 32), 32)

            def grads(a, u, dh):
                sg = jax.nn.sigmoid(a)
                act = a * sg
                return act * u, dh * u * sg * (1.0 + a * (1.0 - sg)), dh * act

            for j in range(0, fm, 128):
                h, da, du = grads(dd[r, j:j + 128].astype(F32), dd[r, S.au + j:S.au + j + 128].astype(F32), dhs[rl, j:j + 128])
                hh[r, j:j + 128] = h.astype(BF)
                dd[r, j:j + 128] = da.astype(BF)
                dd[r, S.au + j:S.au + j + 128] = du.astype(BF)
            both = dd[r, S.at:S.ak].astype(F32)
            h, da, du = grads(both, pltpu.roll(both, 128 - ft, 1), dhs[rl, fm:fm + 128])
            hh[r, S.yt:S.yo] = h.astype(BF)
            rest = jnp.where(lane < ft, da, jnp.where(lane < 2 * ft, pltpu.roll(du, ft, 1), 0.0))
            dd[r, S.at:S.ak] = rest.astype(BF)

    def y_out(slot, ring):
        part = pl.ds(pl.multiple_of(slot * pair + ring * tok, tok), tok)
        dob[...] = dot_nt(yg[part, :], wy[S.yo:S.wy, :]).astype(BF)

    def y_first(slot):
        dhs[...] = dot_nt(yg[slot_rows(slot), :], wy[0:S.yo, :])

    for sub in range(SUBS):
        wait_block(1, 0, 1 - c, sub)
    y_first(0)

    @pl.loop(0, chips)
    def _(slot):
        for sub in range(SUBS):
            wait_block(0, slot, 1 - c, sub)
        fwd_first(slot)

        @pl.when(slot < chips - 1)
        def _():
            pump(0, slot + 1, 1)

        @pl.when(slot == chips - 3)
        def _():
            start_ring(1)

        @pl.when(slot == chips - 1)
        def _():
            pump(1, 1, 0)
        fwd_second(slot)

        @pl.when(slot == 0)
        def _():
            mlp_mid(0)

        @pl.when(slot < chips - 2)
        def _():
            pump(0, slot + 2, 0)

    kc = 256
    sc, dka, dva = stage.at[0, pl.ds(0, tok)], stage.at[1, pl.ds(0, tok)], stage.at[1, pl.ds(tok, tok)]

    def attend(slot, ring, blk, chunks):
        qrow = pl.ds(pl.multiple_of(blk * tok, tok), tok)
        q = qs[qrow, :]
        dout = dob[...]
        srow = pl.ds(pl.multiple_of(slot * pair + ring * tok, tok), tok)
        run = None
        for ch in range(chunks):
            s = dot_nt(q, ks[ch * kc:(ch + 1) * kc, :]) * scale
            if ch >= chunks - 2:
                col = lax.broadcasted_iota(jnp.int32, (tok, kc), 1) + ch * kc
                row = lax.broadcasted_iota(jnp.int32, (tok, kc), 0) + blk * tok
                s = jnp.where(col <= row, s, -jnp.inf)
            sc[:, ch * kc:(ch + 1) * kc] = s
            top = jnp.maximum(s[:, 0:128], s[:, 128:256])
            run = top if run is None else jnp.maximum(run, top)
        m = jnp.max(run, axis=1, keepdims=True)
        tot = jnp.zeros((tok, 128), F32)
        for ch in range(chunks):
            p = jnp.exp(sc[:, ch * kc:(ch + 1) * kc] - m)
            sc[:, ch * kc:(ch + 1) * kc] = p
            tot = tot + p[:, 0:128] + p[:, 128:256]
        inv = 1.0 / jnp.sum(tot, axis=1, keepdims=True)
        for ch in range(chunks):
            p = sc[:, ch * kc:(ch + 1) * kc] * inv
            sc[:, ch * kc:(ch + 1) * kc] = p
            pb[:, ch * kc:(ch + 1) * kc] = p.astype(BF)
        length = chunks * kc
        o = dot_nn(pb[:, 0:length], vs[0:length, :]).astype(BF)
        hh[srow, S.yo:S.wy] = o
        delta = jnp.sum(dout.astype(F32) * o.astype(F32), axis=1, keepdims=True)
        for ch in range(chunks):
            dp = dot_nt(dout, vs[ch * kc:(ch + 1) * kc, :])
            ds[:, ch * kc:(ch + 1) * kc] = (sc[:, ch * kc:(ch + 1) * kc] * (dp - delta)).astype(BF)
        dq = dot_nn(ds[:, 0:length], ks[0:length, :]) * scale
        dd[srow, S.aq:S.at] = dq.astype(BF)
        for ch in range(chunks):
            for acc, lhs, rhs in ((dka, ds, q), (dva, pb, dout)):
                acc[:, ch * kc:(ch + 1) * kc] += dot_tn(rhs, lhs[:, ch * kc:(ch + 1) * kc])

    def attend_ring(slot, ring):
        blk = block_of(slot, ring)
        group = lax.div(blk, 4)
        for v in range(n // 4):
            @pl.when(group == v)
            def _():
                attend(slot, ring, blk, 2 * (v + 1))

    first_core = c == 0
    kv_in = pltpu.make_async_remote_copy(src_ref=ks, dst_ref=kvd, send_sem=k_s.at[0], recv_sem=k_r.at[0],
                                         device_id={"tp": sib}, device_id_type=MESH)

    def kv_own():
        for slot in range(chips):
            for ring in range(2):
                at = pl.multiple_of(block_of(slot, ring) * tok, tok)
                dst = slice(slot * pair + ring * tok, slot * pair + (ring + 1) * tok)
                dk = (dka[:, pl.ds(at, tok)] * scale).astype(BF).T
                dv = dva[:, pl.ds(at, tok)].astype(BF).T
                dd[dst, S.ak:S.av] = dk
                dd[dst, S.av:S.wa] = dv
                qs[pl.ds(at, tok), :] = jnp.where(first_core, dk, dv)
                ks[pl.ds(at, tok), :] = jnp.where(first_core, dv, dk)
        kv_in.start()

    def d_copy(k):
        return pltpu.make_async_remote_copy(
            src_ref=dxs.at[lax.rem(k, 2), pl.ds(pl.multiple_of((1 - c) * tok, tok), tok)], dst_ref=drecv.at[k],
            send_sem=d_s.at[k], recv_sem=d_r.at[k], device_id={"tp": sib}, device_id_type=MESH)

    def dx_main(k, part):
        at = pl.ds(pl.multiple_of(part * (d_model // 2), 1024), d_model // 2)
        out = dot_nn(dd[slot_rows(k + 1), 0:S.ak], wall[0:S.ak, at])
        dxs[k, :, at] = out.astype(BF)

    def dx_kv(k):
        lhs = dd[slice((k + 1) * pair, (k + 2) * pair), S.ak:S.wa]
        for nb in range(0, d_model, 512):
            out = dot_nn(lhs, wall[S.ak:S.wa, nb:nb + 512])
            dxs[k, :, nb:nb + 512] = (dxs[k, :, nb:nb + 512].astype(F32) + out).astype(BF)
        d_copy(jnp.int32(k)).start()

    def dx_part(k):
        buf = lax.rem(k, 2)
        lhs = dd[slot_rows(lax.rem(k + 1, chips)), :]
        for nb in range(0, d_model, 512):
            dxs[buf, :, nb:nb + 512] = dot_nn(lhs, wall[:, nb:nb + 512]).astype(BF)
        d_copy(k).start()

    @pl.loop(0, chips)
    def _(slot):
        y_out(slot, c)
        attend_ring(slot, c)

        @pl.when(jnp.logical_and(slot >= 3, slot < 7))
        def _():
            dx_main(lax.div(slot - 3, 2), lax.rem(slot - 3, 2))

        @pl.when(jnp.logical_and(slot > 0, slot < chips - 1))
        def _():
            pump(1, slot + 1, 0)

        @pl.when(slot > 0)
        def _():
            for sub in range(SUBS):
                wait_block(1, slot, 1 - c, sub)
        y_out(slot, 1 - c)
        attend_ring(slot, 1 - c)

        @pl.when(slot == chips - 1)
        def _():
            kv_own()
            dx_kv(0)

        @pl.when(slot > 0)
        def _():
            y_first(slot)

        @pl.when(jnp.logical_and(slot > 0, slot < chips - 1))
        def _():
            mlp_mid(slot)

        @pl.when(slot < chips - 1)
        def _():
            pump(1, slot + 1, 1)

    place = lax.rem(z, n // S.kv // 2)
    last_place = n // S.kv // 2 - 1
    kv_out = pltpu.make_async_remote_copy(src_ref=kvf, dst_ref=kvg, send_sem=k_s.at[1], recv_sem=k_r.at[1],
                                          device_id={"tp": sib}, device_id_type=MESH)
    parts, lag = KV_PARTS, KV_LAG
    part_rows = S.seq // parts

    def kv_part(i):
        return pl.ds(pl.multiple_of(i * part_rows, part_rows), part_rows)

    def line_copy(way, i):
        src, dst = ((ks, kvl), (vs, kvr))[way]
        to = dev(z + 1) if way == 0 else dev(z - 1)
        return pltpu.make_async_remote_copy(
            src_ref=src.at[kv_part(i)], dst_ref=dst.at[kv_part(i)], send_sem=line_s.at[way, i], recv_sem=line_r.at[way, i],
            device_id={"tp": to}, device_id_type=MESH)

    @pl.when(place == 0)
    def _():
        kvl[...] = jnp.zeros_like(kvl)

    @pl.when(place == last_place)
    def _():
        kvr[...] = jnp.zeros_like(kvr)

    def kv_begin():
        kv_in.wait()
        qs[...] = (qs[...].astype(F32) + kvd[...].astype(F32)).astype(BF)

    def kv_point(p):
        for way in range(2):
            at = place if way == 0 else last_place - place
            i = p + 1 - lag * at
            buf, got = ((ks, kvl), (vs, kvr))[way]

            @pl.when(jnp.logical_and(jnp.logical_and(i >= 0, i < parts), at < last_place))
            def _():
                @pl.when(at > 0)
                def _():
                    line_copy(way, i).wait_recv()
                buf[kv_part(i), :] = (qs[kv_part(i), :].astype(F32) + got[kv_part(i), :].astype(F32)).astype(BF)
                line_copy(way, i).start()

    def kv_sum():
        for way in range(2):
            at = place if way == 0 else last_place - place

            @pl.when(at == last_place)
            def _():
                for i in range(parts):
                    line_copy(way, i).wait_recv()
        kvf[...] = (qs[...].astype(F32) + kvl[...].astype(F32) + kvr[...].astype(F32)).astype(BF)
        kv_out.start()

    def kv_last():
        kv_out.wait()

        @pl.loop(0, chips)
        def _(slot):
            for ring in range(2):
                src = pl.ds(pl.multiple_of(block_of(slot, ring) * tok, tok), tok)
                dst = pl.ds(pl.multiple_of(slot * pair + ring * tok, tok), tok)
                dd[dst, S.ak:S.av] = jnp.where(first_core, kvf[src, :], kvg[src, :])
                dd[dst, S.av:S.wa] = jnp.where(first_core, kvg[src, :], kvf[src, :])
        own = pl.multiple_of(lax.rem(me, n // S.kv) * dwk_out.shape[1], 128)
        out = dot_tn(xg[:, pl.ds(own, dwk_out.shape[1])], dd[:, S.ak:S.wa])
        dhs[:, 0:2 * hd] = out

    def r_copy(k, sub):
        cut_rows = pl.ds(sub * sub_rows, sub_rows)
        return pltpu.make_async_remote_copy(
            src_ref=rsend.at[lax.rem(k, 2), cut_rows], dst_ref=rrecv.at[k + 1, cut_rows],
            send_sem=r_s.at[k, sub], recv_sem=r_r.at[k + 1, sub], device_id={"tp": nxt}, device_id_type=MESH)

    def d_wait(k):
        dref = drecv.at[k]
        pltpu.make_async_remote_copy(
            src_ref=dref, dst_ref=dref, send_sem=d_s.at[0], recv_sem=d_r.at[k],
            device_id={"tp": sib}, device_id_type=MESH).wait_recv()

    def dx_pump(k, sub):
        @pl.when(k > 0)
        def _():
            rref = rrecv.at[k, pl.ds(sub * sub_rows, sub_rows)]
            pltpu.make_async_remote_copy(
                src_ref=rref, dst_ref=rref, send_sem=r_s.at[0, sub], recv_sem=r_r.at[k, sub],
                device_id={"tp": nxt}, device_id_type=MESH).wait_recv()

        @pl.when(k >= 2)
        def _():
            r_copy(k - 2, sub).wait_send()
        buf = lax.rem(k, 2)
        for g in range(0, sub_rows, 16):
            at = pl.ds(sub * sub_rows + g, 16)
            mine = dxs[buf, pl.ds(pl.multiple_of(c * tok + sub * sub_rows + g, 16), 16), :].astype(F32)
            rsend[buf, at, :] = (mine + drecv[k, at, :].astype(F32) + rrecv[k, at, :].astype(F32)).astype(BF)

        @pl.when(k < chips - 2)
        def _():
            r_copy(k, sub).start()

    rows_of = (
        ((wo_out, 0, 0, hd),),
        ((wg_out, 0, 0, kc),), ((wg_out, kc, 0, kc),), ((wg_out, 2 * kc, 0, fm - 2 * kc), (wu_out, 0, fm - 2 * kc, 3 * kc - fm)),
        ((wu_out, 3 * kc - fm, 0, kc),), ((wu_out, 4 * kc - fm, 0, kc),),
        ((wq_out, 0, 0, hd), (wg_out, fm, hd, ft), (wu_out, fm, hd + ft, ft)),
        ((wd_out, 0, 0, kc),), ((wd_out, kc, 0, kc),), ((wd_out, 2 * kc, 0, fm - 2 * kc), (wd_out, fm, fm - 2 * kc, ft)),
    )
    units, x_end = len(rows_of), 7

    def g_copies(u):
        return [pltpu.make_async_copy(stage.at[u % 2, pl.ds(src, size)], ref.at[pl.ds(dst, size)], gsem.at[u % 2, i])
                for i, (ref, dst, src, size) in enumerate(rows_of[u])]

    def dw_unit(u):
        for w in range(2, units):
            @pl.when(u == w)
            def _():
                for cp in g_copies(w - 2):
                    cp.wait()
        buf = lax.rem(u, 2)

        @pl.when(u == 0)
        def _():
            for nb in range(0, d_model, kc):
                stage[0, 0:hd, nb:nb + kc] = dot_tn(hh[:, S.yo:S.wy], yg[:, nb:nb + kc])
        for lhs, rhs, lo, hi in ((dd, xg, 1, x_end), (hh, yg, x_end, units)):
            @pl.when(jnp.logical_and(u >= lo, u < hi))
            def _():
                at = pl.ds(pl.multiple_of((u - lo) * kc, kc), kc)
                for nb in range(0, d_model, kc):
                    stage[buf, :, nb:nb + kc] = dot_tn(lhs[:, at], rhs[:, nb:nb + kc])
        for w in range(units):
            @pl.when(u == w)
            def _():
                for cp in g_copies(w):
                    cp.start()

    own_k = chips - 1

    def own_tokens():
        d_wait(own_k)
        for g in range(0, tok, 16):
            mine = dxs[own_k % 2, pl.ds(pl.multiple_of(c * tok + g, 16), 16), :].astype(F32)
            pb[g:g + 16, :] = (mine + drecv[own_k, g:g + 16, :].astype(F32)).astype(BF)

    last = [pltpu.make_async_copy(pb, dx_own, osem.at[0]),
            pltpu.make_async_copy(dhs.at[:, pl.ds(0, hd)], dwk_out.at[0], osem.at[1]),
            pltpu.make_async_copy(dhs.at[:, pl.ds(hd, hd)], dwv_out.at[0], osem.at[2]),
            pltpu.make_async_copy(rsend.at[(own_k - 1) % 2, pl.ds(0, sub_rows)], dx_send.at[pl.ds(0, sub_rows)], osem.at[4]),
            pltpu.make_async_copy(rsend.at[(own_k - 1) % 2, pl.ds(sub_rows, sub_rows)], dx_send.at[pl.ds(sub_rows, sub_rows)],
                                  osem.at[3])]

    kv_begin()
    kv_point(-1)
    kv_point(0)

    @pl.loop(0, chips - 1)
    def _(k):
        d_wait(k)
        dx_pump(k, 0)
        kv_point(2 * k + 1)

        @pl.when(k == 0)
        def _():
            dx_kv(1)
            mlp_mid(chips - 1)

        @pl.when(k >= 1)
        def _():
            d_copy(k - 1).wait_send()
            dx_part(k + 1)

        @pl.when(jnp.logical_and(k >= 2, k < chips - 3))
        def _():
            dw_unit(2 * k - 1)

        @pl.when(k == chips - 2)
        def _():
            last[3].start()
            kv_last()
            last[1].start()
            last[2].start()
            own_tokens()
            last[0].start()
        dx_pump(k, 1)
        kv_point(2 * k + 2)

        @pl.loop(0, jnp.where(k == 0, 2, jnp.where(k < chips - 2, 1, 0)))
        def _(i):
            dw_unit(jnp.where(k == 0, i, jnp.minimum(2 * k, units - 1)))

        @pl.when(k == chips - 3)
        def _():
            kv_sum()

    last[4].start()
    for cp in last:
        cp.wait()

    for way in range(2):
        at = place if way == 0 else last_place - place

        @pl.when(at < last_place)
        def _():
            for i in range(parts):
                line_copy(way, i).wait_send()
    for sub in range(SUBS):
        r_copy(chips - 3, sub).wait_send()
    for k in range(chips - 2, chips):
        d_copy(k).wait_send()

    for st in range(2):
        for sem, count in ((ring_s, chips - 1), (sib_s, chips)):
            span_all = gathered[st].at[pl.ds(0, count * tok)]
            pltpu.make_async_remote_copy(
                src_ref=span_all, dst_ref=span_all, send_sem=sem.at[st], recv_sem=rsem.at[st, 0, 0, 0],
                device_id={"tp": sib}, device_id_type=MESH).wait_send()
    for u in range(units - 2, units):
        for cp in g_copies(u):
            cp.wait()


def finish_kernel(wg_hbm, wu_hbm, wd_hbm, wo_hbm, wq_hbm, dwk_hbm, dwv_hbm,
                  wg_out, wu_out, wd_out, wo_out, wq_out, dwk_out, dwv_out,
                  big, wov, wqv, wqt, kvb, isem, osem):
    half = big.shape[1] // 2
    moves = [(wq_hbm, wqv, None, None)]
    for w, (src, dst) in enumerate(((wg_hbm, wg_out), (wu_hbm, wu_out), (wd_hbm, wd_out))):
        for r in (0, half):
            moves.append((src.at[pl.ds(r, half)], big.at[w, pl.ds(r, half)], big.at[w, pl.ds(r, half)], dst.at[pl.ds(r, half)]))
    moves += [(wo_hbm, wov, wov, wo_out), (dwk_hbm, kvb.at[0], kvb.at[0], dwk_out), (dwv_hbm, kvb.at[1], kvb.at[1], dwv_out)]
    moves[0] = (wq_hbm, wqv, wqt, wq_out)
    into = [pltpu.make_async_copy(m[0], m[1], isem.at[i]) for i, m in enumerate(moves)]
    out = [pltpu.make_async_copy(m[2], m[3], osem.at[i]) for i, m in enumerate(moves)]
    for cp in into:
        cp.start()
    for i in range(len(moves)):
        into[i].wait()
        if i == 0:
            wqt[...] = wqv[...].T
        out[i].start()
    for cp in out:
        cp.wait()


def solution(mesh):
    n_dev = mesh.shape["tp"]

    def local_step(x_loc, dy_loc, w_q, w_k, w_v, w_o, w_gate, w_up, w_down):
        tok, d_model = x_loc.shape
        ff, hd, kv = w_gate.shape[1], w_q.shape[2], w_k.shape[1]
        S = Sizes(n_dev, kv, tok, d_model, ff, hd)
        seq, chips, pair = S.seq, S.chips, S.pair
        any_spec = pl.BlockSpec(memory_space=pl.ANY)
        dma = pltpu.SemaphoreType.DMA
        reps = n_dev // kv
        dcut = d_model // reps
        ff_out, hd_out = jax.ShapeDtypeStruct((ff, d_model), F32), jax.ShapeDtypeStruct((hd, d_model), F32)
        kv_out = jax.ShapeDtypeStruct((1, dcut, hd), F32)
        outs = pl.pallas_call(
            functools.partial(fused_kernel, S),
            out_shape=(
                jax.ShapeDtypeStruct((tok, d_model), BF),
                jax.ShapeDtypeStruct((tok, d_model), BF),
                kv_out, kv_out, ff_out, ff_out, hd_out, ff_out, hd_out,
            ),
            in_specs=[any_spec] * 9,
            out_specs=[any_spec] * 9,
            scratch_shapes=[
                pltpu.VMEM((seq, d_model), BF), pltpu.VMEM((seq, d_model), BF),
                pltpu.VMEM((S.wa, d_model), BF), pltpu.VMEM((S.wy, d_model), BF),
                pltpu.VMEM((seq, S.wa), BF), pltpu.VMEM((seq, S.wy), BF), pltpu.VMEM((pair, S.fm + 128), F32), pltpu.VMEM((tok, hd), BF),
                pltpu.VMEM((seq, hd), BF), pltpu.VMEM((seq, hd), BF), pltpu.VMEM((seq, hd), BF),
                pltpu.VMEM((tok, seq), BF), pltpu.VMEM((tok, seq), BF),
                pltpu.VMEM((d_model, hd), BF), pltpu.VMEM((2, d_model, kv, hd), BF), pltpu.VMEM((kv * 256, hd), F32),
                pltpu.VMEM((2, pair, d_model), BF), pltpu.VMEM((2, tok, d_model), BF),
                pltpu.VMEM((chips, tok, d_model), BF), pltpu.VMEM((chips, tok, d_model), BF),
                pltpu.VMEM((seq, hd), BF), pltpu.VMEM((seq, hd), BF), pltpu.VMEM((seq, hd), BF),
                pltpu.VMEM((seq, hd), BF), pltpu.VMEM((seq, hd), BF),
                pltpu.VMEM((2, 2 * hd, d_model), F32),
                dma((10,)), dma((2,)), dma((2,)), dma((2, chips, 2, SUBS)), dma((2,)), dma((5,)),
                dma((2, 3)), dma((chips,)), dma((chips,)), dma((chips, SUBS)), dma((chips, SUBS)), dma((2,)), dma((2,)),
                dma((2, KV_PARTS)), dma((2, KV_PARTS)),
            ],
            compiler_params=pltpu.CompilerParams(collective_id=0, has_side_effects=True, vmem_limit_bytes=67043328),
            name="fused",
        )(x_loc, dy_loc, w_q[:, 0, :], w_k, w_v, w_o[0], w_gate.T, w_up.T, w_down)
        dx_own, dx_send, dwk, dwv, wg, wu, wq, wd, wo = outs
        hop = [(i, (i + 2 - 4 * (i % 2)) % n_dev) for i in range(n_dev)]
        dx_last = lax.ppermute(dx_send, "tp", hop)
        wg, wu, wd, wo, wq, dwk, dwv = pl.pallas_call(
            finish_kernel,
            in_specs=[any_spec] * 7,
            out_specs=[any_spec] * 7,
            out_shape=(ff_out, ff_out, ff_out, hd_out, jax.ShapeDtypeStruct((d_model, hd), F32), kv_out, kv_out),
            scratch_shapes=[
                pltpu.VMEM((3, ff, d_model), F32), pltpu.VMEM((hd, d_model), F32), pltpu.VMEM((hd, d_model), F32),
                pltpu.VMEM((d_model, hd), F32), pltpu.VMEM((2, 1, dcut, hd), F32), dma((10,)), dma((10,)),
            ],
            cost_estimate=pl.CostEstimate(flops=10 ** 10, bytes_accessed=38 * 10 ** 6, transcendentals=0),
            compiler_params=pltpu.CompilerParams(vmem_limit_bytes=62 << 20),
            name="finish",
        )(wg, wu, wd, wo, wq, dwk, dwv)
        dx = (dx_own.astype(F32) + dx_last.astype(F32)).astype(BF)
        return (dx, wq.reshape(d_model, 1, hd), dwk, dwv, wo[None], wg.T, wu.T, wd)

    token_spec = P(("dp", "tp"), None)
    in_specs = (token_spec, token_spec, P(None, "tp", None), P(None, None, None), P(None, None, None),
                P("tp", None, None), P(None, "tp"), P(None, "tp"), P("tp", None))
    out_specs = (token_spec, P("dp", "tp", None), P(("dp", "tp"), None, None), P(("dp", "tp"), None, None),
                 P(("dp", "tp"), None, None), P("dp", "tp"), P("dp", "tp"), P(("dp", "tp"), None))
    return jax.shard_map(local_step, mesh=mesh, in_specs=in_specs, out_specs=out_specs, check_vma=False)
```
